128 devices in a mesh: row: 8 (over x, z_hi), col: 16 (over y, z_lo, core).
Axes of the slice: x: 4, y: 4, z: 4 (z_hi: 2, z_lo: 2; z = z_hi * 2 + z_lo), core: 2. Of those that a mesh axis runs over, the one named last changes fastest.
Arguments:
- pair_act: float32 [768, 768, 128], P('row', 'col'), may hold values from -6 to 6
- grad_out: float32 [768, 768, 128], P('row', 'col'), may hold values from -6 to 6
- residue_mask: int32 [768], replicated, may hold values from 0 to 1, as said below
- norm_gains: float32 [2, 128], replicated, may hold values from 0.25 to 1.75
- weights: float32 [6, 128, 128], replicated, may hold values from -0.5 to 0.5
Outputs:
- grad_pair: float32 [768, 768, 128], P('row', 'col')
- grad_weights: float32 [6, 128, 128], replicated
- grad_gains: float32 [2, 128], replicated
The draws below stay inside these ranges and needn't reach their ends.
Inputs may be any that keep to these rules, and one draw needn't show every extreme that they name: `residue_mask`: the residues form four stretches of 192; in each stretch the valid residues are a prefix of at least 96 and fewer than 192 residues.
All inputs are finite; a program needn't handle non-finite values.
Results may differ from the reference program's by a relative error of at most 0.00009.
Values sent between devices are 32-bit elements; how exact they have to be, the bound alone decides.
A program may use at most 128 MiB of HBM per device.

```python
import jax
import jax.numpy as jnp
from jax import lax

C = 128
N = 768


def draw_residue_mask(key, part):
    stretch = N // 4
    subkeys = jax.random.split(jax.random.fold_in(key, 17), 1)
    lengths = jax.random.randint(subkeys[0], (4,), stretch // 2, stretch)
    position = jnp.arange(N) % stretch
    stretch_id = jnp.arange(N) // stretch
    return (position < lengths[stretch_id]).astype(jnp.int32)


def shard_levels(key, shape, cuts, low, largest):
    factor_of = 1.0
    for dim, shards_of in cuts:
        draws = jax.random.uniform(jax.random.fold_in(jax.random.fold_in(key, 6), dim), (shards_of,), jnp.float32, low / len(cuts), largest / len(cuts))
        factor_of = factor_of * jnp.repeat(jnp.exp(draws), shape[dim] // shards_of).reshape((-1,) + (1,) * (len(shape) - 1 - dim))
    return factor_of


def normal_values(stream_key, dims, width, reach, shards=(), dtype=jnp.bfloat16):
    drawn = width * jax.random.normal(stream_key, dims, jnp.float32)
    if shards:
        drawn = drawn * shard_levels(stream_key, dims, shards, -0.22, 0.18)
    return jnp.clip(drawn, -reach, reach).astype(dtype)


def setup_inputs(seed: int = 0) -> dict:
    key_list = jax.random.split(jax.random.key(seed), 6)
    pair_act = normal_values(key_list[0], (N, N, C), 1.0, 6.0, ((0, 8), (1, 16)), jnp.float32)
    grad_out = normal_values(key_list[1], (N, N, C), 1.0, 6.0, ((0, 8), (1, 16)), jnp.float32)
    residue_mask = draw_residue_mask(jax.random.fold_in(key_list[5], 71), 0)
    norm_gains = jnp.clip(1.0 + 0.15 * jax.random.normal(key_list[3], (2, C), jnp.float32), 0.25, 1.75)
    weights = normal_values(key_list[4], (6, C, C), C ** -0.5, 0.5, (), jnp.float32)
    return {"pair_act": pair_act, "grad_out": grad_out, "residue_mask": residue_mask, "norm_gains": norm_gains, "weights": weights}


epsilon = 1e-05
block_rows = 32
highest = lax.Precision.HIGHEST

def norm_parts(operand):
    average = lax.optimization_barrier(jnp.mean(operand, axis=-1, keepdims=True))
    centered = operand - average
    inv_std = lax.rsqrt(lax.optimization_barrier(jnp.mean(centered * centered, axis=-1, keepdims=True)) + epsilon)
    return (centered * inv_std, inv_std)

def norm_back(grad_hat, normed, inv_std):
    first_mean = lax.optimization_barrier(jnp.mean(grad_hat, axis=-1, keepdims=True))
    second_mean = lax.optimization_barrier(jnp.mean(grad_hat * normed, axis=-1, keepdims=True))
    return inv_std * (grad_hat - first_mean - normed * second_mean)

def project(operand, weight):
    return jnp.einsum('ijc,cd->ijd', operand, weight, precision=highest)

def sigmoid(operand):
    return 1.0 / (1.0 + jnp.exp(-operand))

def input_side(pair_rows, mask_rows, residue_mask, norm_gains, weights):
    pair_hat, inv_std = norm_parts(pair_rows)
    normed = pair_hat * norm_gains[0]
    pair_mask = (mask_rows[:, None] * residue_mask[None, :]).astype(jnp.float32)[:, :, None]
    lin_a = project(normed, weights[0])
    sig_a = sigmoid(project(normed, weights[1]))
    lin_b = project(normed, weights[2])
    sig_b = sigmoid(project(normed, weights[3]))
    return (pair_hat, inv_std, normed, pair_mask, lin_a, sig_a, lin_b, sig_b)

def output_side(normed, tri_rows, grad_rows, norm_gains, weights):
    tri_hat, tri_inv = norm_parts(tri_rows)
    tri_norm = tri_hat * norm_gains[1]
    lin_o = project(tri_norm, weights[5])
    sig_g = sigmoid(project(normed, weights[4]))
    d_out = grad_rows * sig_g
    d_gate = grad_rows * lin_o * sig_g * (1.0 - sig_g)
    d_norm = project(d_out, weights[5].T)
    d_tri = norm_back(d_norm * norm_gains[1], tri_hat, tri_inv)
    return (tri_hat, tri_norm, d_out, d_gate, d_norm, d_tri)

def reference(pair_act, grad_out, residue_mask, norm_gains, weights):
    residues = pair_act.shape[0]
    channels = pair_act.shape[2]
    blocks = residues // block_rows
    full_shape = pair_act.shape
    block_shape = (blocks, block_rows, residues, channels)
    mask_blocks = residue_mask.reshape(blocks, block_rows)

    def first_pass(inputs_block):
        pair_rows, mask_rows = inputs_block
        sides = input_side(pair_rows, mask_rows, residue_mask, norm_gains, weights)
        pair_mask = sides[3]
        return (pair_mask * sides[5] * sides[4], pair_mask * sides[7] * sides[6])
    act_a, act_b = lax.map(first_pass, (pair_act.reshape(block_shape), mask_blocks))
    act_a = act_a.reshape(full_shape)
    act_b = act_b.reshape(full_shape)
    triangle = jnp.einsum('ikc,jkc->ijc', act_a, act_b, precision=highest)

    def second_pass(inputs_block):
        pair_rows, tri_rows, grad_rows = inputs_block
        pair_hat, inv_std = norm_parts(pair_rows)
        normed = pair_hat * norm_gains[0]
        outside = output_side(normed, tri_rows, grad_rows, norm_gains, weights)
        tri_hat, tri_norm, d_out, d_norm, d_tri = (outside[0], outside[1], outside[2], outside[4], outside[5])
        grad_o = jnp.einsum('ijc,ijd->cd', tri_norm, d_out, precision=highest)
        gain_two = lax.optimization_barrier(jnp.sum(d_norm * tri_hat, axis=(0, 1)))
        return (d_tri, grad_o, gain_two)
    d_tri, grad_o, gain_two = lax.map(second_pass, (pair_act.reshape(block_shape), triangle.reshape(block_shape), grad_out.reshape(block_shape)))
    d_tri = d_tri.reshape(full_shape)
    grad_o = lax.optimization_barrier(jnp.sum(grad_o, axis=0))
    gain_two = lax.optimization_barrier(jnp.sum(gain_two, axis=0))
    d_act_a = jnp.einsum('ijc,jkc->ikc', d_tri, act_b, precision=highest)
    d_act_b = jnp.einsum('ijc,ikc->jkc', d_tri, act_a, precision=highest)

    def third_pass(inputs_block):
        pair_rows, mask_rows, tri_rows, grad_rows, da_rows, db_rows = inputs_block
        pair_hat, inv_std, normed, pair_mask, lin_a, sig_a, lin_b, sig_b = input_side(pair_rows, mask_rows, residue_mask, norm_gains, weights)
        d_gate = output_side(normed, tri_rows, grad_rows, norm_gains, weights)[3]
        d_lin_a = da_rows * pair_mask * sig_a
        d_sig_a = da_rows * pair_mask * lin_a * sig_a * (1.0 - sig_a)
        d_lin_b = db_rows * pair_mask * sig_b
        d_sig_b = db_rows * pair_mask * lin_b * sig_b * (1.0 - sig_b)
        d_normed = project(d_lin_a, weights[0].T) + project(d_sig_a, weights[1].T)
        d_normed = d_normed + project(d_lin_b, weights[2].T) + project(d_sig_b, weights[3].T)
        d_normed = d_normed + project(d_gate, weights[4].T)
        weight_grads = jnp.stack([jnp.einsum('ijc,ijd->cd', normed, d_lin_a, precision=highest), jnp.einsum('ijc,ijd->cd', normed, d_sig_a, precision=highest), jnp.einsum('ijc,ijd->cd', normed, d_lin_b, precision=highest), jnp.einsum('ijc,ijd->cd', normed, d_sig_b, precision=highest), jnp.einsum('ijc,ijd->cd', normed, d_gate, precision=highest)])
        gain_one = lax.optimization_barrier(jnp.sum(d_normed * pair_hat, axis=(0, 1)))
        grad_rows_pair = norm_back(d_normed * norm_gains[0], pair_hat, inv_std)
        return (grad_rows_pair, weight_grads, gain_one)
    grad_pair, weight_grads, gain_one = lax.map(third_pass, (pair_act.reshape(block_shape), mask_blocks, triangle.reshape(block_shape), grad_out.reshape(block_shape), d_act_a.reshape(block_shape), d_act_b.reshape(block_shape)))
    grad_pair = grad_pair.reshape(full_shape)
    weight_grads = lax.optimization_barrier(jnp.sum(weight_grads, axis=0))
    gain_one = lax.optimization_barrier(jnp.sum(gain_one, axis=0))
    grad_weights = jnp.concatenate([weight_grads, grad_o[None]], axis=0) / residues
    grad_gains = jnp.stack([gain_one, gain_two]) / residues
    return (grad_pair, grad_weights, grad_gains)
```

```python
import functools

import jax
import jax.numpy as jnp
from jax import lax
from jax.experimental import pallas as pl
from jax.experimental.pallas import tpu as pltpu
from jax.sharding import PartitionSpec as P

EPS = 1e-05
F32 = jnp.float32
BF16 = jnp.bfloat16
MESH = pl.DeviceIdType.MESH
VLIM = 60 * 2**20


def params(**kw):
    return pltpu.CompilerParams(vmem_limit_bytes=VLIM, **kw)


def split(v):
    hi = v.astype(BF16)
    lo = (v - hi.astype(F32)).astype(BF16)
    return hi, lo


def dot3(lhs, rhs, dims):
    (lh, ll), (rh, rl) = lhs, rhs
    d = functools.partial(
        lax.dot_general, dimension_numbers=(dims, ((), ())), preferred_element_type=F32
    )
    return d(lh, rh) + (d(lh, rl) + d(ll, rh))


NN = ((1,), (0,))
NT = ((1,), (1,))
TN = ((0,), (0,))


def place():
    row = lax.axis_index("row")
    col = lax.axis_index("col")
    return row // 2, col // 4, lax.rem(row, 2) * 2 + lax.rem(col // 2, 2), lax.rem(col, 2)


def partner(spot, step):
    x, y, z, core = spot
    a, b, c, d = step
    x = lax.rem(x + a, 4)
    y = lax.rem(y + b, 4)
    z = lax.rem(z + c, 4)
    core = lax.rem(core + d, 2)
    return x * 2 + z // 2, y * 4 + lax.rem(z, 2) * 2 + core


def steps():
    out = []
    for s in range(1, 128):
        o = (s * 45) % 128
        out.append((o // 2 % 4, o // 8 % 4, o // 32, o % 2))
    return out


def exchange_kernel(count, *refs):
    srcs = refs[:count]
    dsts = refs[count : 2 * count]
    send_sem, recv_sem = refs[2 * count :]
    spot = place()
    me = lax.axis_index("row") * 16 + lax.axis_index("col")
    barrier = pltpu.get_barrier_semaphore()
    for step in steps():
        r, q = partner(spot, step)
        pl.semaphore_signal(
            barrier, inc=1, device_id={"row": r, "col": q}, device_id_type=MESH
        )
    pl.semaphore_wait(barrier, 127)
    for n in range(count):
        own = pltpu.make_async_copy(
            srcs[n].at[pl.ds(me, 1), :], dsts[n].at[pl.ds(me, 1), :], recv_sem.at[n]
        )
        own.start()
        for step in steps():
            r, q = partner(spot, step)
            to = r * 16 + q
            pltpu.make_async_remote_copy(
                src_ref=srcs[n].at[pl.ds(to, 1), :],
                dst_ref=dsts[n].at[pl.ds(me, 1), :],
                send_sem=send_sem.at[n],
                recv_sem=recv_sem.at[n],
                device_id={"row": r, "col": q},
                device_id_type=MESH,
            ).start()
    for n in range(count):
        pltpu.make_async_copy(srcs[n], dsts[n], recv_sem.at[n]).wait()
        pltpu.make_async_copy(
            srcs[n].at[pl.ds(0, 120), :], dsts[n].at[pl.ds(0, 120), :], send_sem.at[n]
        ).wait()
        for row in range(120, 127):
            pltpu.make_async_copy(
                srcs[n].at[pl.ds(row, 1), :], dsts[n].at[pl.ds(row, 1), :], send_sem.at[n]
            ).wait()


def exchange(ident, *arrays):
    count = len(arrays)
    return pl.pallas_call(
        functools.partial(exchange_kernel, count),
        out_shape=[jax.ShapeDtypeStruct(a.shape, a.dtype) for a in arrays],
        in_specs=[pl.BlockSpec(memory_space=pl.ANY)] * count,
        out_specs=[pl.BlockSpec(memory_space=pl.ANY)] * count,
        scratch_shapes=[pltpu.SemaphoreType.DMA((count,))] * 2,
        compiler_params=params(collective_id=ident, has_side_effects=True),
        name=f"exchange_{ident}",
    )(*arrays)


def sum_kernel(x_ref, out_ref, parts, mine, send_a, recv_a, send_b, recv_b):
    spot = place()
    me = lax.axis_index("row") * 16 + lax.axis_index("col")
    barrier = pltpu.get_barrier_semaphore()
    for step in steps():
        r, q = partner(spot, step)
        pl.semaphore_signal(
            barrier, inc=1, device_id={"row": r, "col": q}, device_id_type=MESH
        )
    pl.semaphore_wait(barrier, 127)

    def rows_of(owner):
        return pl.ds(pl.multiple_of(owner * 8, 8), 8)

    for step in steps():
        r, q = partner(spot, step)
        to = r * 16 + q
        pltpu.make_async_remote_copy(
            src_ref=x_ref.at[rows_of(to), :],
            dst_ref=parts.at[rows_of(me), :],
            send_sem=send_a,
            recv_sem=recv_a,
            device_id={"row": r, "col": q},
            device_id_type=MESH,
        ).start()
    pltpu.make_async_copy(x_ref.at[rows_of(me), :], parts.at[rows_of(me), :], recv_a).start()
    pltpu.make_async_copy(x_ref, parts, recv_a).wait()
    total = parts[...].reshape(128, 8, 128).sum(0)
    mine[...] = total
    for step in steps():
        r, q = partner(spot, step)
        pltpu.make_async_remote_copy(
            src_ref=mine,
            dst_ref=out_ref.at[rows_of(me), :],
            send_sem=send_b,
            recv_sem=recv_b,
            device_id={"row": r, "col": q},
            device_id_type=MESH,
        ).start()
    pltpu.make_async_copy(mine, out_ref.at[rows_of(me), :], recv_b).start()
    pltpu.make_async_copy(x_ref, out_ref, recv_b).wait()
    some = x_ref.at[pl.ds(0, 127 * 8), :]
    into = parts.at[pl.ds(0, 127 * 8), :]
    pltpu.make_async_copy(some, into, send_a).wait()
    pltpu.make_async_copy(some, into, send_b).wait()


def sum_everywhere(ident, x):
    return pl.pallas_call(
        sum_kernel,
        out_shape=jax.ShapeDtypeStruct(x.shape, x.dtype),
        in_specs=[pl.BlockSpec(memory_space=pl.ANY)],
        out_specs=pl.BlockSpec(memory_space=pl.ANY),
        scratch_shapes=[pltpu.VMEM((1024, 128), F32), pltpu.VMEM((8, 128), F32)]
        + [pltpu.SemaphoreType.DMA] * 4,
        compiler_params=params(collective_id=ident, has_side_effects=True),
        name="sum_everywhere",
    )(x)


def turn_in(ref):
    rows = ref.shape[0]
    flat = ref.reshape(rows * 8, 128)
    parts = [flat[pl.ds(j, rows, stride=8), :] for j in range(8)]
    return jnp.concatenate(parts, axis=0).T


def norm_parts(v):
    scale = 1.0 / v.shape[0]
    mu = jnp.sum(v, axis=0, keepdims=True) * scale
    cen = v - mu
    inv = lax.rsqrt(jnp.sum(cen * cen, axis=0, keepdims=True) * scale + EPS)
    return cen * inv, inv


def norm_back(h, hat, inv):
    scale = 1.0 / h.shape[0]
    m1 = jnp.sum(h, axis=0, keepdims=True) * scale
    m2 = jnp.sum(h * hat, axis=0, keepdims=True) * scale
    return inv * (h - m1 - hat * m2)


def sigmoid(v):
    return 1.0 / (1.0 + jnp.exp(-v))


def front_kernel(x_ref, mask_ref, gain_ref, wh_ref, wl_ref, *outs):
    a_ref, b_ref, hat_ref, inv_ref, la_ref, sa_ref, lb_ref, sb_ref, sg_ref = outs
    hat, inv = norm_parts(turn_in(x_ref))
    hat_ref[...] = hat
    inv_ref[...] = inv
    normed = split(hat * gain_ref[:, 0:1])
    mask = mask_ref[...]

    def proj(n):
        rows = pl.ds(n * 128, 128)
        return dot3((wh_ref[rows, :], wl_ref[rows, :]), normed, NN)

    lin = proj(0)
    sig = sigmoid(proj(1))
    la_ref[...] = lin
    sa_ref[...] = sig
    a_ref[...] = mask * sig * lin
    lin = proj(2)
    sig = sigmoid(proj(3))
    lb_ref[...] = lin
    sb_ref[...] = sig
    b_ref[...] = mask * sig * lin
    sg_ref[...] = sigmoid(proj(4))


def middle_kernel(t_ref, go_ref, sg_ref, gain_ref, wh_ref, wl_ref, uh_ref, ul_ref, *outs):
    dt_ref, dg_ref, ow_ref, gt_ref = outs
    tri_hat, tri_inv = norm_parts(t_ref[...])
    gain = gain_ref[:, 1:2]
    tri_norm = split(tri_hat * gain)
    lin_o = dot3((wh_ref[...], wl_ref[...]), tri_norm, NN)
    sig = sg_ref[...]
    d_out = turn_in(go_ref) * sig
    dg_ref[...] = d_out * lin_o * (1.0 - sig)
    d_out = split(d_out)
    d_norm = dot3((uh_ref[...], ul_ref[...]), d_out, NN)
    dt_ref[...] = norm_back(d_norm * gain, tri_hat, tri_inv)

    @pl.when(pl.program_id(0) == 0)
    def _():
        ow_ref[...] = jnp.zeros_like(ow_ref)
        gt_ref[...] = jnp.zeros_like(gt_ref)

    ow_ref[...] += dot3(tri_norm, d_out, NT)
    prod = d_norm * tri_hat
    gt_ref[...] += sum(prod[:, 128 * t : 128 * t + 128] for t in range(6))


def back_kernel(
    da_ref, db_ref, mask_ref, hat_ref, inv_ref, la_ref, sa_ref, lb_ref, sb_ref, dg_ref,
    gain_ref, uh_ref, ul_ref, gp_ref, gw_ref, go_ref,
):
    mask = mask_ref[...]
    hat = hat_ref[...]
    gain = gain_ref[:, 0:1]
    normed = split(hat * gain)

    @pl.when(pl.program_id(0) == 0)
    def _():
        gw_ref[...] = jnp.zeros_like(gw_ref)
        go_ref[...] = jnp.zeros_like(go_ref)

    total = None

    def use(n, grad):
        nonlocal total
        grad = split(grad)
        gw_ref[pl.ds(n * 128, 128), :] += dot3(normed, grad, NT)
        rows = pl.ds(n * 128, 128)
        term = dot3((uh_ref[rows, :], ul_ref[rows, :]), grad, NN)
        total = term if total is None else total + term

    for n, d_ref, l_ref, s_ref in ((0, da_ref, la_ref, sa_ref), (2, db_ref, lb_ref, sb_ref)):
        sig = s_ref[...]
        d_lin = d_ref[...] * mask * sig
        use(n, d_lin)
        use(n + 1, d_lin * l_ref[...] * (1.0 - sig))
    use(4, dg_ref[...])
    prod = total * hat
    go_ref[...] += sum(prod[:, 128 * t : 128 * t + 128] for t in range(6))
    grad = norm_back(total * gain, hat, inv_ref[...]).T
    rows = gp_ref.shape[0]
    flat = gp_ref.reshape(rows * 8, 128)
    for j in range(8):
        flat[pl.ds(j, rows, stride=8), :] = grad[j * rows : (j + 1) * rows, :]


CHUNK = 768
STEPS = 6


def chunked(rows=128):
    return pl.BlockSpec((rows, CHUNK), lambda s: (0, s))


def whole(*shape):
    return pl.BlockSpec(shape, lambda s: (0,) * len(shape))


TILE_SPEC = pl.BlockSpec((96, None, 8, 128), lambda s: (0, s, 0, 0))
FULL = jax.ShapeDtypeStruct((128, 4608), F32)


def front(pair4, mask, gains_t, wh, wl):
    return pl.pallas_call(
        front_kernel,
        grid=(STEPS,),
        in_specs=[TILE_SPEC, chunked(1), whole(128, 2), whole(640, 128), whole(640, 128)],
        out_specs=[chunked()] * 3 + [chunked(1)] + [chunked()] * 5,
        out_shape=[FULL] * 3 + [jax.ShapeDtypeStruct((1, 4608), F32)] + [FULL] * 5,
        compiler_params=params(),
        name="front",
    )(pair4, mask, gains_t, wh, wl)


def middle(tri, go4, sig_g, gains_t, wh, wl, uh, ul):
    return pl.pallas_call(
        middle_kernel,
        grid=(STEPS,),
        in_specs=[chunked(), TILE_SPEC, chunked(), whole(128, 2)] + [whole(128, 128)] * 4,
        out_specs=[chunked(), chunked(), whole(128, 128), whole(128, 128)],
        out_shape=[FULL, FULL] + [jax.ShapeDtypeStruct((128, 128), F32)] * 2,
        compiler_params=params(),
        name="middle",
    )(tri, go4, sig_g, gains_t, wh, wl, uh, ul)


def back(da, db, mask, hat, inv, la, sa, lb, sb, dg, gains_t, uh, ul):
    return pl.pallas_call(
        back_kernel,
        grid=(STEPS,),
        in_specs=[chunked(), chunked(), chunked(1), chunked(), chunked(1)]
        + [chunked()] * 5
        + [whole(128, 2), whole(640, 128), whole(640, 128)],
        out_specs=[TILE_SPEC, whole(640, 128), whole(128, 128)],
        out_shape=[
            jax.ShapeDtypeStruct((96, 6, 8, 128), F32),
            jax.ShapeDtypeStruct((640, 128), F32),
            jax.ShapeDtypeStruct((128, 128), F32),
        ],
        compiler_params=params(),
        name="back",
    )(da, db, mask, hat, inv, la, sa, lb, sb, dg, gains_t, uh, ul)


def swap_four(blocks):
    lane = lax.broadcasted_iota(jnp.int32, blocks[0].shape, 1)
    outs = []
    for a in range(4):
        out = None
        for b in range(4):
            shift = (96 * (b - a)) % 384
            moved = blocks[b] if shift == 0 else pltpu.roll(blocks[b], shift, 1)
            out = moved if out is None else jnp.where(lane < 96 * b, out, moved)
        outs.append(out)
    return outs


def read_group(ref, group, half):
    lanes = pl.ds(pl.multiple_of(group * 384, 384), 384)
    return [ref[pl.ds((half * 4 + r) * 16, 16), lanes] for r in range(4)]


def write_group(ref, group, half, blocks):
    lanes = pl.ds(pl.multiple_of(group * 384, 384), 384)
    for r in range(4):
        ref[pl.ds((half * 4 + r) * 16, 16), lanes] = blocks[r]


def gather_matrix(src_ref, hi_ref, lo_ref):
    @pl.loop(0, 12)
    def _(group):
        for half in range(2):
            for k, block in enumerate(swap_four(read_group(src_ref, group, half))):
                hi, lo = split(block)
                rows = pl.ds(pl.multiple_of(group * 64 + k * 16, 16), 16)
                lanes = pl.ds(half * 384, 384)
                hi_ref[rows, lanes] = hi
                lo_ref[rows, lanes] = lo


PITCH = 56


def triangle_kernel(ra_ref, rb_ref, ah_ref, al_ref, bh_ref, bl_ref, out_ref, scr):
    gather_matrix(ra_ref, ah_ref, al_ref)
    gather_matrix(rb_ref, bh_ref, bl_ref)

    @pl.loop(0, 3)
    def _(n):
        lanes = pl.ds(pl.multiple_of(n * 256, 256), 256)
        res = dot3((bh_ref[...], bl_ref[...]), (ah_ref[:, lanes], al_ref[:, lanes]), TN)
        for t in range(2):
            for q in range(16):
                scr[n * 2 + t, pl.ds(q * PITCH, 48), :] = res[
                    q * 48 : q * 48 + 48, t * 128 : t * 128 + 128
                ]

    @pl.loop(0, 12)
    def _(group):
        for half in range(2):
            blocks = []
            for k in range(4):
                parts = [
                    scr.at[half * 3 + t][pl.ds(group * 4 + k, 16, stride=PITCH), :]
                    for t in range(3)
                ]
                blocks.append(jnp.concatenate(parts, axis=1))
            write_group(out_ref, group, half, swap_four(blocks))


def triangle(ra, rb):
    mat = jax.ShapeDtypeStruct((768, 768), BF16)
    return pl.pallas_call(
        triangle_kernel,
        out_shape=[mat] * 4 + [FULL],
        in_specs=[pl.BlockSpec(memory_space=pltpu.VMEM)] * 2,
        out_specs=[pl.BlockSpec(memory_space=pltpu.VMEM)] * 5,
        scratch_shapes=[pltpu.VMEM((6, 16 * PITCH, 128), F32)],
        compiler_params=params(),
        name="triangle",
    )(ra, rb)


def grads_kernel(rd_ref, ah_ref, al_ref, bh_ref, bl_ref, oa_ref, ob_ref, scr, dh, dl, res):
    @pl.loop(0, 12)
    def _(group):
        for half in range(2):
            for k, block in enumerate(swap_four(read_group(rd_ref, group, half))):
                for t in range(3):
                    scr.at[half * 3 + t][pl.ds(group * 4 + k, 16, stride=PITCH), :] = block[
                        :, t * 128 : t * 128 + 128
                    ]

    @pl.loop(0, 16)
    def _(q):
        for t in range(6):
            hi, lo = split(scr[t, pl.ds(pl.multiple_of(q * PITCH, 8), 48), :])
            rows = pl.ds(pl.multiple_of(q * 48, 16), 48)
            dh[rows, pl.ds(t * 128, 128)] = hi
            dl[rows, pl.ds(t * 128, 128)] = lo

    def spread(out_ref):
        @pl.loop(0, 12)
        def _(group):
            for half in range(2):
                blocks = [
                    res[
                        pl.ds(pl.multiple_of(group * 64 + k * 16, 16), 16),
                        pl.ds(half * 384, 384),
                    ]
                    for k in range(4)
                ]
                write_group(out_ref, group, half, swap_four(blocks))

    @pl.loop(0, 3)
    def _(n):
        lanes = pl.ds(pl.multiple_of(n * 256, 256), 256)
        res[:, lanes] = dot3((bh_ref[...], bl_ref[...]), (dh[:, lanes], dl[:, lanes]), NN)

    spread(oa_ref)

    @pl.loop(0, 3)
    def _(n):
        lanes = pl.ds(pl.multiple_of(n * 256, 256), 256)
        res[:, lanes] = dot3((ah_ref[...], al_ref[...]), (dh[lanes, :], dl[lanes, :]), NT)

    spread(ob_ref)


def act_grads(rd, ah, al, bh, bl):
    return pl.pallas_call(
        grads_kernel,
        out_shape=[FULL] * 2,
        in_specs=[pl.BlockSpec(memory_space=pltpu.VMEM)] * 5,
        out_specs=[pl.BlockSpec(memory_space=pltpu.VMEM)] * 2,
        scratch_shapes=[
            pltpu.VMEM((6, 16 * PITCH, 128), F32),
            pltpu.VMEM((768, 768), BF16),
            pltpu.VMEM((768, 768), BF16),
            pltpu.VMEM((768, 768), F32),
        ],
        compiler_params=params(),
        name="act_grads",
    )(rd, ah, al, bh, bl)


def round_split(v):
    hi = lax.reduce_precision(v, 8, 7)
    return hi.astype(BF16), (v - hi).astype(BF16)


def on_device(pair_act, grad_out, residue_mask, norm_gains, weights):
    tile_rows, tile_cols, channels = pair_act.shape
    residues = residue_mask.shape[0]
    row_mask = lax.dynamic_slice_in_dim(
        residue_mask, lax.axis_index("row") * tile_rows, tile_rows
    )
    col_mask = lax.dynamic_slice_in_dim(
        residue_mask, lax.axis_index("col") * tile_cols, tile_cols
    )
    mask = (col_mask[:, None] * row_mask[None, :]).astype(F32).reshape(1, -1)
    gains_t = norm_gains.T
    turned = jnp.transpose(weights, (0, 2, 1))
    wh, wl = round_split(turned.reshape(6 * channels, channels))
    uh, ul = round_split(weights.reshape(6 * channels, channels))
    cut = 5 * channels
    pair4 = pair_act.reshape(tile_rows, tile_cols // 8, 8, channels)
    go4 = grad_out.reshape(tile_rows, tile_cols // 8, 8, channels)
    a, b, hat, inv, la, sa, lb, sb, sg = front(pair4, mask, gains_t, wh[:cut], wl[:cut])
    ra, rb = exchange(0, a, b)
    ah, al, bh, bl, tri = triangle(ra, rb)
    (rt,) = exchange(1, tri)
    dt, dg, out_part, gain_two = middle(
        rt, go4, sg, gains_t, wh[cut:], wl[cut:], uh[cut:], ul[cut:]
    )
    (rd,) = exchange(2, dt)
    oa, ob = act_grads(rd, ah, al, bh, bl)
    da, db = exchange(3, oa, ob)
    grad_pair, weight_part, gain_one = back(
        da, db, mask, hat, inv, la, sa, lb, sb, dg, gains_t, uh[:cut], ul[:cut]
    )
    gains = jnp.stack([gain_one, gain_two]).sum(-1)
    spare = jnp.zeros((1024 - 6 * channels - 2, channels), F32)
    combined = jnp.concatenate([weight_part, out_part, gains, spare], axis=0)
    total = sum_everywhere(4, combined) / residues
    return (
        grad_pair.reshape(pair_act.shape),
        total[: 6 * channels].reshape(6, channels, channels),
        total[6 * channels : 6 * channels + 2],
    )


def solution(mesh):
    return jax.shard_map(
        on_device,
        mesh=mesh,
        in_specs=(P("row", "col", None), P("row", "col", None), P(), P(), P()),
        out_specs=(P("row", "col", None), P(), P()),
        check_vma=False,
    )
```

```python
import functools

import jax
import jax.numpy as jnp
from jax import lax
from jax.experimental import pallas as pl
from jax.experimental.pallas import tpu as pltpu
from jax.sharding import PartitionSpec as P

EPS = 1e-05
F32 = jnp.float32
BF16 = jnp.bfloat16
MESH = pl.DeviceIdType.MESH
VLIM = 60 * 2**20


def params(**kw):
    return pltpu.CompilerParams(vmem_limit_bytes=VLIM, **kw)


def split(v):
    hi = v.astype(BF16)
    lo = (v - hi.astype(F32)).astype(BF16)
    return hi, lo


def dot3(lhs, rhs, dims):
    (lh, ll), (rh, rl) = lhs, rhs
    d = functools.partial(
        lax.dot_general, dimension_numbers=(dims, ((), ())), preferred_element_type=F32
    )
    return d(lh, rh) + (d(lh, rl) + d(ll, rh))


NN = ((1,), (0,))
NT = ((1,), (1,))
TN = ((0,), (0,))


def place():
    row = lax.axis_index("row")
    col = lax.axis_index("col")
    return row // 2, col // 4, lax.rem(row, 2) * 2 + lax.rem(col // 2, 2), lax.rem(col, 2)


def partner(spot, step):
    x, y, z, core = spot
    a, b, c, d = step
    x = lax.rem(x + a, 4)
    y = lax.rem(y + b, 4)
    z = lax.rem(z + c, 4)
    core = lax.rem(core + d, 2)
    return x * 2 + z // 2, y * 4 + lax.rem(z, 2) * 2 + core


def steps():
    out = []
    for s in range(1, 128):
        o = (s * 45) % 128
        out.append((o // 2 % 4, o // 8 % 4, o // 32, o % 2))
    return out


def row_of(ref, row, lanes):
    return ref.at[pl.ds(row, 1), lanes]


def send_all(src, dst, lanes, send_sem, recv_sem):
    spot = place()
    me = lax.axis_index("row") * 16 + lax.axis_index("col")
    for step in steps():
        r, q = partner(spot, step)
        pltpu.make_async_remote_copy(
            src_ref=row_of(src, r * 16 + q, lanes),
            dst_ref=row_of(dst, me, lanes),
            send_sem=send_sem,
            recv_sem=recv_sem,
            device_id={"row": r, "col": q},
            device_id_type=MESH,
        ).start()
    dst[pl.ds(me, 1), lanes] = src[pl.ds(me, 1), lanes]


def wait_all(tally, part, sem):
    some = tally.at[pl.ds(0, 127 * (part[1] - part[0]))]
    pltpu.make_async_copy(some, some, sem).wait()


def sum_kernel(x_ref, out_ref, parts, mine, send_a, recv_a, send_b, recv_b):
    spot = place()
    me = lax.axis_index("row") * 16 + lax.axis_index("col")
    barrier = pltpu.get_barrier_semaphore()
    for step in steps():
        r, q = partner(spot, step)
        pl.semaphore_signal(
            barrier, inc=1, device_id={"row": r, "col": q}, device_id_type=MESH
        )
    pl.semaphore_wait(barrier, 127)

    def rows_of(owner):
        return pl.ds(pl.multiple_of(owner * 8, 8), 8)

    for step in steps():
        r, q = partner(spot, step)
        to = r * 16 + q
        pltpu.make_async_remote_copy(
            src_ref=x_ref.at[rows_of(to), :],
            dst_ref=parts.at[rows_of(me), :],
            send_sem=send_a,
            recv_sem=recv_a,
            device_id={"row": r, "col": q},
            device_id_type=MESH,
        ).start()
    pltpu.make_async_copy(x_ref.at[rows_of(me), :], parts.at[rows_of(me), :], recv_a).start()
    pltpu.make_async_copy(x_ref, parts, recv_a).wait()
    total = parts[...].reshape(128, 8, 128).sum(0)
    mine[...] = total
    for step in steps():
        r, q = partner(spot, step)
        pltpu.make_async_remote_copy(
            src_ref=mine,
            dst_ref=out_ref.at[rows_of(me), :],
            send_sem=send_b,
            recv_sem=recv_b,
            device_id={"row": r, "col": q},
            device_id_type=MESH,
        ).start()
    pltpu.make_async_copy(mine, out_ref.at[rows_of(me), :], recv_b).start()
    pltpu.make_async_copy(x_ref, out_ref, recv_b).wait()
    some = x_ref.at[pl.ds(0, 127 * 8), :]
    into = parts.at[pl.ds(0, 127 * 8), :]
    pltpu.make_async_copy(some, into, send_a).wait()
    pltpu.make_async_copy(some, into, send_b).wait()


def sum_everywhere(ident, x):
    return pl.pallas_call(
        sum_kernel,
        out_shape=jax.ShapeDtypeStruct(x.shape, x.dtype),
        in_specs=[pl.BlockSpec(memory_space=pl.ANY)],
        out_specs=pl.BlockSpec(memory_space=pl.ANY),
        scratch_shapes=[pltpu.VMEM((1024, 128), F32), pltpu.VMEM((8, 128), F32)]
        + [pltpu.SemaphoreType.DMA] * 4,
        compiler_params=params(collective_id=ident, has_side_effects=True),
        name="sum_everywhere",
    )(x)


def turn_in(ref):
    rows = ref.shape[0]
    flat = ref.reshape(rows * 8, 128)
    parts = [flat[pl.ds(j, rows, stride=8), :] for j in range(8)]
    return jnp.concatenate(parts, axis=0).T


def norm_parts(v):
    scale = 1.0 / v.shape[0]
    mu = jnp.sum(v, axis=0, keepdims=True) * scale
    cen = v - mu
    inv = lax.rsqrt(jnp.sum(cen * cen, axis=0, keepdims=True) * scale + EPS)
    return cen * inv, inv


def norm_back(h, hat, inv):
    scale = 1.0 / h.shape[0]
    m1 = jnp.sum(h, axis=0, keepdims=True) * scale
    m2 = jnp.sum(h * hat, axis=0, keepdims=True) * scale
    return inv * (h - m1 - hat * m2)


def sigmoid(v):
    return 1.0 / (1.0 + jnp.exp(-v))


def swap_four(blocks):
    lane = lax.broadcasted_iota(jnp.int32, blocks[0].shape, 1)
    outs = []
    for a in range(4):
        out = None
        for b in range(4):
            shift = (96 * (b - a)) % 384
            moved = blocks[b] if shift == 0 else pltpu.roll(blocks[b], shift, 1)
            out = moved if out is None else jnp.where(lane < 96 * b, out, moved)
        outs.append(out)
    return outs


def read_group(ref, group, half):
    lanes = pl.ds(pl.multiple_of(group * 384, 384), 384)
    return [ref[pl.ds((half * 4 + r) * 16, 16), lanes] for r in range(4)]


def write_group(ref, group, half, blocks):
    lanes = pl.ds(pl.multiple_of(group * 384, 384), 384)
    for r in range(4):
        ref[pl.ds((half * 4 + r) * 16, 16), lanes] = blocks[r]


PITCH = 56
UNIT = 1536


def lanes_of(part):
    return pl.ds(part[0] * UNIT, (part[1] - part[0]) * UNIT)


def groups_of(part):
    return pl.loop(part[0] * 4, part[1] * 4)


def chunks_of(part):
    return pl.loop(part[0] * 2, part[1] * 2)


def rows_of(part):
    return pl.ds(part[0] * 256, (part[1] - part[0]) * 256)


def gather_matrix(src_ref, hi_ref, lo_ref, part):
    @groups_of(part)
    def _(group):
        for half in range(2):
            for k, block in enumerate(swap_four(read_group(src_ref, group, half))):
                hi, lo = split(block)
                rows = pl.ds(pl.multiple_of(group * 64 + k * 16, 16), 16)
                lanes = pl.ds(half * 384, 384)
                hi_ref[rows, lanes] = hi
                lo_ref[rows, lanes] = lo


def spread_pitched(scr, out_ref, part):
    @groups_of(part)
    def _(group):
        for half in range(2):
            blocks = []
            for k in range(4):
                pieces = [
                    scr.at[half * 3 + t][pl.ds(group * 4 + k, 16, stride=PITCH), :]
                    for t in range(3)
                ]
                blocks.append(jnp.concatenate(pieces, axis=1))
            write_group(out_ref, group, half, swap_four(blocks))


def spread_rows(res, out_ref, part):
    @groups_of(part)
    def _(group):
        for half in range(2):
            blocks = [
                res[
                    pl.ds(pl.multiple_of(group * 64 + k * 16, 16), 16),
                    pl.ds(half * 384, 384),
                ]
                for k in range(4)
            ]
            write_group(out_ref, group, half, swap_four(blocks))


def gather_pitched(src_ref, scr, part):
    @groups_of(part)
    def _(group):
        for half in range(2):
            for k, block in enumerate(swap_four(read_group(src_ref, group, half))):
                for t in range(3):
                    scr.at[half * 3 + t][pl.ds(group * 4 + k, 16, stride=PITCH), :] = block[
                        :, t * 128 : t * 128 + 128
                    ]


A_PARTS = ((0, 2), (2, 3))
T_PARTS = ((0, 2), (2, 3))
D_PARTS = ((0, 2), (2, 3))
DA_PARTS = ((0, 1), (1, 3))
DB_PARTS = ((0, 2), (2, 3))
ALL = (0, 3)
SENDS = 11


def step_kernel(
    pair_hbm, go_hbm, mask_ref, gain_ref, w_ref, gp_hbm, gw_ref, ow_ref, g1_ref, g2_ref,
    xin, gin, s1, s2, r1, r2, r3, hat_ref, inv_ref, nh, nl, la, sa, lb, sb, sg, dg,
    ah, al, bh, bl, dh, dl, res, scr, th, tl, uh, ul, tally,
    in_sem, go_sem, out_sem, send_sem, recv_sem,
):
    spot = place()
    for s in range(6):
        pltpu.make_async_copy(pair_hbm.at[:, s], xin.at[s], in_sem.at[s]).start()
    for s in range(6):
        pltpu.make_async_copy(go_hbm.at[:, s], gin.at[s], go_sem.at[s]).start()
    barrier = pltpu.get_barrier_semaphore()
    for step in steps():
        r, q = partner(spot, step)
        pl.semaphore_signal(
            barrier, inc=1, device_id={"row": r, "col": q}, device_id_type=MESH
        )
    for n in range(6):
        rows = pl.ds(n * 128, 128)
        th[rows, :], tl[rows, :] = split(w_ref[n].T)
        uh[rows, :], ul[rows, :] = split(w_ref[n])
    gw_ref[...] = jnp.zeros_like(gw_ref)
    ow_ref[...] = jnp.zeros_like(ow_ref)
    g1_ref[...] = jnp.zeros_like(g1_ref)
    g2_ref[...] = jnp.zeros_like(g2_ref)
    gain_in = gain_ref[:, 0:1]
    gain_tri = gain_ref[:, 1:2]

    def wide(s):
        return pl.ds(pl.multiple_of(s * 768, 768), 768)

    def weight(n, hi=th, lo=tl):
        rows = pl.ds(n * 128, 128)
        return hi[rows, :], lo[rows, :]

    def side(n, lanes, lin_ref, sig_ref, out_ref):
        normed = (nh[:, lanes], nl[:, lanes])
        lin = dot3(weight(n), normed, NN)
        sig = sigmoid(dot3(weight(n + 1), normed, NN))
        lin_ref[:, lanes] = lin
        sig_ref[:, lanes] = sig
        out_ref[:, lanes] = mask_ref[:, lanes] * sig * lin

    @chunks_of(ALL)
    def _(s):
        lanes = wide(s)
        pltpu.make_async_copy(pair_hbm.at[:, s], xin.at[s], in_sem.at[s]).wait()
        hat, inv = norm_parts(turn_in(xin.at[s]))
        hat_ref[:, lanes] = hat
        inv_ref[:, lanes] = inv
        nh[:, lanes], nl[:, lanes] = split(hat * gain_in)
        side(2, lanes, lb, sb, s2)

    pl.semaphore_wait(barrier, 127)
    which = iter(range(SENDS))

    def send(src, dst, part):
        n = next(which)
        lanes = lanes_of(part)
        send_all(src, dst, lanes, send_sem.at[n], recv_sem.at[n])
        return (
            lambda: wait_all(tally, part, send_sem.at[n]),
            lambda: wait_all(tally, part, recv_sem.at[n]),
        )

    b_out, b_in = send(s2, r2, ALL)
    moves = []
    for part in A_PARTS:

        @chunks_of(part)
        def _(s):
            side(0, wide(s), la, sa, s1)

        moves.append(send(s1, r1, part))

    @chunks_of(ALL)
    def _(s):
        lanes = wide(s)
        sg[:, lanes] = sigmoid(dot3(weight(4), (nh[:, lanes], nl[:, lanes]), NN))

    b_in()
    gather_matrix(r2, bh, bl, ALL)
    for i, part in enumerate(A_PARTS):
        moves[i][1]()
        gather_matrix(r1, ah, al, part)
        rows = rows_of(part)

        @pl.loop(0, 3)
        def _(n):
            lanes = pl.ds(pl.multiple_of(n * 256, 256), 256)
            got = dot3((bh[rows, :], bl[rows, :]), (ah[rows, lanes], al[rows, lanes]), TN)
            if i > 0:
                got = got + res[:, lanes]
            if i < len(A_PARTS) - 1:
                res[:, lanes] = got
            else:
                for t in range(2):
                    for q in range(16):
                        scr[n * 2 + t, pl.ds(q * PITCH, 48), :] = got[
                            q * 48 : q * 48 + 48, t * 128 : t * 128 + 128
                        ]

    for out, _in in moves:
        out()
    moves = []
    for part in T_PARTS:
        spread_pitched(scr, s1, part)
        moves.append(send(s1, r3, part))

    b_out()
    later = []
    for i, part in enumerate(D_PARTS):
        moves[i][1]()

        @chunks_of(part)
        def _(s):
            lanes = wide(s)
            pltpu.make_async_copy(go_hbm.at[:, s], gin.at[s], go_sem.at[s]).wait()
            tri_hat, tri_inv = norm_parts(r3[:, lanes])
            tri_norm = split(tri_hat * gain_tri)
            lin_o = dot3(weight(5), tri_norm, NN)
            sig = sg[:, lanes]
            d_out = turn_in(gin.at[s]) * sig
            dg[:, lanes] = d_out * lin_o * (1.0 - sig)
            d_out = split(d_out)
            d_norm = dot3(weight(5, uh, ul), d_out, NN)
            s2[:, lanes] = norm_back(d_norm * gain_tri, tri_hat, tri_inv)
            ow_ref[...] += dot3(tri_norm, d_out, NT)
            prod = d_norm * tri_hat
            g2_ref[...] += sum(prod[:, 128 * t : 128 * t + 128] for t in range(6))

        later.append(send(s2, r2, part))

    def use(n, lanes, grad):
        grad = split(grad)
        rows = pl.ds(n * 128, 128)
        gw_ref[rows, :] += dot3((nh[:, lanes], nl[:, lanes]), grad, NT)
        return dot3(weight(n, uh, ul), grad, NN)

    @chunks_of(ALL)
    def _(s):
        lanes = wide(s)
        sg[:, lanes] = use(4, lanes, dg[:, lanes])

    for i, part in enumerate(D_PARTS):
        later[i][1]()
        gather_pitched(r2, scr, part)

    @pl.loop(0, 16)
    def _(q):
        for t in range(6):
            hi, lo = split(scr[t, pl.ds(pl.multiple_of(q * PITCH, 8), 48), :])
            rows = pl.ds(pl.multiple_of(q * 48, 16), 48)
            dh[rows, pl.ds(t * 128, 128)] = hi
            dl[rows, pl.ds(t * 128, 128)] = lo

    for out, _in in moves:
        out()
    moves_a = []
    for part in DA_PARTS:
        rows = rows_of(part)

        @pl.loop(0, 3)
        def _(n):
            lanes = pl.ds(pl.multiple_of(n * 256, 256), 256)
            res[rows, lanes] = dot3((bh[rows, :], bl[rows, :]), (dh[:, lanes], dl[:, lanes]), NN)

        spread_rows(res, s1, part)
        moves_a.append(send(s1, r1, part))
    for out, _in in later:
        out()
    moves_b = []
    for part in DB_PARTS:
        rows = rows_of(part)

        @pl.loop(0, 3)
        def _(n):
            lanes = pl.ds(pl.multiple_of(n * 256, 256), 256)
            res[rows, lanes] = dot3((ah[rows, :], al[rows, :]), (dh[lanes, :], dl[lanes, :]), NT)

        spread_rows(res, s2, part)
        moves_b.append(send(s2, r3, part))

    def back(n, lanes, d_ref, lin_ref, sig_ref):
        sig = sig_ref[:, lanes]
        d_lin = d_ref[:, lanes] * mask_ref[:, lanes] * sig
        first = use(n, lanes, d_lin)
        return first + use(n + 1, lanes, d_lin * lin_ref[:, lanes] * (1.0 - sig))

    for i, part in enumerate(DA_PARTS):
        moves_a[i][1]()

        @chunks_of(part)
        def _(s):
            lanes = wide(s)
            sg[:, lanes] += back(0, lanes, r1, la, sa)

    for i, part in enumerate(DB_PARTS):
        moves_b[i][1]()

        @chunks_of(part)
        def _(s):
            lanes = wide(s)
            total = sg[:, lanes] + back(2, lanes, r3, lb, sb)
            hat = hat_ref[:, lanes]
            prod = total * hat
            g1_ref[...] += sum(prod[:, 128 * t : 128 * t + 128] for t in range(6))
            grad = norm_back(total * gain_in, hat, inv_ref[:, lanes]).T
            flat = xin.at[s].reshape(768, 128)
            for j in range(8):
                flat[pl.ds(j, 96, stride=8), :] = grad[j * 96 : (j + 1) * 96, :]
            pltpu.make_async_copy(xin.at[s], gp_hbm.at[:, s], out_sem.at[s]).start()

    for out, _in in moves_a + moves_b:
        out()
    for s in range(6):
        pltpu.make_async_copy(xin.at[s], gp_hbm.at[:, s], out_sem.at[s]).wait()


def whole_step(pair4, go4, mask, gains_t, weights):
    vmem = pl.BlockSpec(memory_space=pltpu.VMEM)
    hbm = pl.BlockSpec(memory_space=pl.ANY)
    full = pltpu.VMEM((128, 4608), F32)
    half = pltpu.VMEM((128, 4608), BF16)
    mat = pltpu.VMEM((768, 768), BF16)
    wts = pltpu.VMEM((768, 128), BF16)
    tiles = pltpu.VMEM((6, 96, 8, 128), F32)
    dma = pltpu.SemaphoreType.DMA
    square = jax.ShapeDtypeStruct((128, 128), F32)
    return pl.pallas_call(
        step_kernel,
        in_specs=[hbm, hbm, vmem, vmem, vmem],
        out_specs=[hbm, vmem, vmem, vmem, vmem],
        out_shape=[
            jax.ShapeDtypeStruct((96, 6, 8, 128), F32),
            jax.ShapeDtypeStruct((640, 128), F32),
            square,
            square,
            square,
        ],
        scratch_shapes=[tiles, tiles, full, full, full, full, full, full]
        + [pltpu.VMEM((1, 4608), F32), half, half]
        + [full] * 6
        + [mat] * 6
        + [pltpu.VMEM((768, 768), F32), pltpu.VMEM((6, 16 * PITCH, 128), F32)]
        + [wts] * 4
        + [pltpu.VMEM((381, 12, 128), F32)]
        + [dma((6,)), dma((6,)), dma((6,)), dma((SENDS,)), dma((SENDS,))],
        compiler_params=params(collective_id=0, has_side_effects=True),
        name="whole_step",
    )(pair4, go4, mask, gains_t, weights)


def on_device(pair_act, grad_out, residue_mask, norm_gains, weights):
    tile_rows, tile_cols, channels = pair_act.shape
    residues = residue_mask.shape[0]
    row_mask = lax.dynamic_slice_in_dim(
        residue_mask, lax.axis_index("row") * tile_rows, tile_rows
    )
    col_mask = lax.dynamic_slice_in_dim(
        residue_mask, lax.axis_index("col") * tile_cols, tile_cols
    )
    mask = (col_mask[:, None] * row_mask[None, :]).astype(F32).reshape(1, -1)
    gains_t = norm_gains.T
    pair4 = pair_act.reshape(tile_rows, tile_cols // 8, 8, channels)
    go4 = grad_out.reshape(tile_rows, tile_cols // 8, 8, channels)
    grad_pair, weight_part, out_part, gain_one, gain_two = whole_step(
        pair4, go4, mask, gains_t, weights
    )
    gains = jnp.stack([gain_one, gain_two]).sum(-1)
    spare = jnp.zeros((1024 - 6 * channels - 2, channels), F32)
    combined = jnp.concatenate([weight_part, out_part, gains, spare], axis=0)
    total = sum_everywhere(1, combined) / residues
    return (
        grad_pair.reshape(pair_act.shape),
        total[: 6 * channels].reshape(6, channels, channels),
        total[6 * channels : 6 * channels + 2],
    )


def solution(mesh):
    return jax.shard_map(
        on_device,
        mesh=mesh,
        in_specs=(P("row", "col", None), P("row", "col", None), P(), P(), P()),
        out_specs=(P("row", "col", None), P(), P()),
        check_vma=False,
    )
```

```python
import functools

import jax
import jax.numpy as jnp
from jax import lax
from jax.experimental import pallas as pl
from jax.experimental.pallas import tpu as pltpu
from jax.sharding import PartitionSpec as P

EPS = 1e-05
F32 = jnp.float32
BF16 = jnp.bfloat16
MESH = pl.DeviceIdType.MESH
VLIM = 60 * 2**20


def params(**kw):
    return pltpu.CompilerParams(vmem_limit_bytes=VLIM, **kw)


def split(v):
    hi = v.astype(BF16)
    lo = (v - hi.astype(F32)).astype(BF16)
    return hi, lo


def dot3(lhs, rhs, dims):
    (lh, ll), (rh, rl) = lhs, rhs
    d = functools.partial(
        lax.dot_general, dimension_numbers=(dims, ((), ())), preferred_element_type=F32
    )
    return d(lh, rh) + (d(lh, rl) + d(ll, rh))


NN = ((1,), (0,))
NT = ((1,), (1,))
TN = ((0,), (0,))


def place():
    row = lax.axis_index("row")
    col = lax.axis_index("col")
    return row // 2, col // 4, lax.rem(row, 2) * 2 + lax.rem(col // 2, 2), lax.rem(col, 2)


def partner(spot, step):
    x, y, z, core = spot
    a, b, c, d = step
    x = lax.rem(x + a, 4)
    y = lax.rem(y + b, 4)
    z = lax.rem(z + c, 4)
    core = lax.rem(core + d, 2)
    return x * 2 + z // 2, y * 4 + lax.rem(z, 2) * 2 + core


def steps():
    out = []
    for s in range(1, 128):
        o = (s * 45) % 128
        out.append((o // 2 % 4, o // 8 % 4, o // 32, o % 2))
    return out


def row_of(ref, row, lanes):
    return ref.at[pl.ds(row, 1), lanes]


def send_all(src, dst, lanes, send_sem, recv_sem):
    spot = place()
    me = lax.axis_index("row") * 16 + lax.axis_index("col")
    for step in steps():
        r, q = partner(spot, step)
        pltpu.make_async_remote_copy(
            src_ref=row_of(src, r * 16 + q, lanes),
            dst_ref=row_of(dst, me, lanes),
            send_sem=send_sem,
            recv_sem=recv_sem,
            device_id={"row": r, "col": q},
            device_id_type=MESH,
        ).start()
    dst[pl.ds(me, 1), lanes] = src[pl.ds(me, 1), lanes]


def wait_all(tally, part, sem):
    some = tally.at[pl.ds(0, 127 * (part[1] - part[0]))]
    pltpu.make_async_copy(some, some, sem).wait()


def chip_at(spot, a, b, c):
    x, y, z, _ = spot
    return lax.rem(x + a, 4), lax.rem(y + b, 4), lax.rem(z + c, 4)


def device_at(x, y, z, core):
    return x * 2 + z // 2, y * 4 + lax.rem(z, 2) * 2 + core


def eight(tile):
    return pl.ds(pl.multiple_of(tile * 8, 8), 8)


def tile_copy(src, dst, send_sem, recv_sem, device):
    return pltpu.make_async_remote_copy(
        src_ref=src,
        dst_ref=dst,
        send_sem=send_sem,
        recv_sem=recv_sem,
        device_id={"row": device[0], "col": device[1]},
        device_id_type=MESH,
    )


def wait_tiles(ref, count, sem):
    some = ref.at[pl.ds(0, count * 8), :]
    pltpu.make_async_copy(some, some, sem).wait()


def settle(small, large, tiles, owner, send_sem, recv_sem, n):
    @pl.when(owner)
    def _():
        if tiles > 1:
            wait_tiles(small, tiles - 1, send_sem.at[n])
            wait_tiles(small, tiles - 1, recv_sem.at[n + 1])
        wait_tiles(large, 127, send_sem.at[n + 1])

    @pl.when(jnp.logical_not(owner))
    def _():
        wait_tiles(small, tiles, send_sem.at[n])
        wait_tiles(small, tiles, recv_sem.at[n + 1])


CHIPS = [(o // 16, o // 4 % 4, o % 4) for o in [(s * 27) % 64 for s in range(64)]]


def turn_in(ref):
    rows = ref.shape[0]
    flat = ref.reshape(rows * 8, 128)
    parts = [flat[pl.ds(j, rows, stride=8), :] for j in range(8)]
    return jnp.concatenate(parts, axis=0).T


def norm_parts(v):
    scale = 1.0 / v.shape[0]
    mu = jnp.sum(v, axis=0, keepdims=True) * scale
    cen = v - mu
    inv = lax.rsqrt(jnp.sum(cen * cen, axis=0, keepdims=True) * scale + EPS)
    return cen * inv, inv


def norm_back(h, hat, inv):
    scale = 1.0 / h.shape[0]
    m1 = jnp.sum(h, axis=0, keepdims=True) * scale
    m2 = jnp.sum(h * hat, axis=0, keepdims=True) * scale
    return inv * (h - m1 - hat * m2)


def sigmoid(v):
    return 1.0 / (1.0 + jnp.exp(-v))


def swap_four(blocks):
    lane = lax.broadcasted_iota(jnp.int32, blocks[0].shape, 1)
    outs = []
    for a in range(4):
        out = None
        for b in range(4):
            shift = (96 * (b - a)) % 384
            moved = blocks[b] if shift == 0 else pltpu.roll(blocks[b], shift, 1)
            out = moved if out is None else jnp.where(lane < 96 * b, out, moved)
        outs.append(out)
    return outs


def read_group(ref, group, half):
    lanes = pl.ds(pl.multiple_of(group * 384, 384), 384)
    return [ref[pl.ds((half * 4 + r) * 16, 16), lanes] for r in range(4)]


def write_group(ref, group, half, blocks):
    lanes = pl.ds(pl.multiple_of(group * 384, 384), 384)
    for r in range(4):
        ref[pl.ds((half * 4 + r) * 16, 16), lanes] = blocks[r]


PITCH = 56
UNIT = 768


def lanes_of(part):
    return pl.ds(part[0] * UNIT, (part[1] - part[0]) * UNIT)


def groups_of(part):
    return pl.loop(part[0] * 2, part[1] * 2)


def chunks_of(part):
    return pl.loop(part[0], part[1])


def rows_of(part):
    return pl.ds(part[0] * 128, (part[1] - part[0]) * 128)


def gather_matrix(src_ref, hi_ref, lo_ref, part):
    @groups_of(part)
    def _(group):
        for half in range(2):
            for k, block in enumerate(swap_four(read_group(src_ref, group, half))):
                hi, lo = split(block)
                rows = pl.ds(pl.multiple_of(group * 64 + k * 16, 16), 16)
                lanes = pl.ds(half * 384, 384)
                hi_ref[rows, lanes] = hi
                lo_ref[rows, lanes] = lo


def spread_pitched(scr, out_ref, part):
    @groups_of(part)
    def _(group):
        for half in range(2):
            blocks = []
            for k in range(4):
                pieces = [
                    scr.at[half * 3 + t][pl.ds(group * 4 + k, 16, stride=PITCH), :]
                    for t in range(3)
                ]
                blocks.append(jnp.concatenate(pieces, axis=1))
            write_group(out_ref, group, half, swap_four(blocks))


def spread_rows(res, out_ref, part):
    @groups_of(part)
    def _(group):
        for half in range(2):
            blocks = [
                res[
                    pl.ds(pl.multiple_of(group * 64 + k * 16, 16), 16),
                    pl.ds(half * 384, 384),
                ]
                for k in range(4)
            ]
            write_group(out_ref, group, half, swap_four(blocks))


def gather_pitched(src_ref, scr, part):
    @groups_of(part)
    def _(group):
        for half in range(2):
            for k, block in enumerate(swap_four(read_group(src_ref, group, half))):
                for t in range(3):
                    scr.at[half * 3 + t][pl.ds(group * 4 + k, 16, stride=PITCH), :] = block[
                        :, t * 128 : t * 128 + 128
                    ]


B_PARTS = ((0, 2), (2, 6))
A_PARTS = ((0, 4), (4, 6))
T_PARTS = ((0, 2), (2, 4), (4, 6))
DA_PARTS = ((0, 2), (2, 6))
DB_PARTS = ((0, 3), (3, 5), (5, 6))
ALL = (0, 6)
SENDS = 15


def step_kernel(
    pair_hbm, go_hbm, valid_ref, gain_ref, w_ref, gp_hbm, wo_ref, go_ref,
    xin, gin, s1, s2, r1, r2, r3, hat_ref, inv_ref, nh, nl, la, sa, lb, sb, sg, dg,
    ah, al, bh, bl, dh, dl, res, scr, th, tl, uh, ul, tally,
    mask_ref, gw_ref, g1_ref, g2_ref, gains, parts1, parts2, mine,
    in_sem, go_sem, out_sem, send_sem, recv_sem, sum_send, sum_recv,
):
    spot = place()
    for s in range(6):
        pltpu.make_async_copy(pair_hbm.at[:, s], xin.at[s], in_sem.at[s]).start()
    for s in range(6):
        pltpu.make_async_copy(go_hbm.at[:, s], gin.at[s], go_sem.at[s]).start()
    barrier = pltpu.get_barrier_semaphore()
    for step in steps():
        r, q = partner(spot, step)
        pl.semaphore_signal(
            barrier, inc=1, device_id={"row": r, "col": q}, device_id_type=MESH
        )
    for n in range(6):
        rows = pl.ds(n * 128, 128)
        th[rows, :], tl[rows, :] = split(w_ref[n].T)
        uh[rows, :], ul[rows, :] = split(w_ref[n])
    gw_ref[...] = jnp.zeros_like(gw_ref)
    g1_ref[...] = jnp.zeros_like(g1_ref)
    g2_ref[...] = jnp.zeros_like(g2_ref)
    for n in range(2):
        gains[n] = jnp.broadcast_to(gain_ref[n : n + 1, :], (128, 128)).T
    gain_in = gains[0, :, 0:1]
    gain_tri = gains[1, :, 0:1]
    me = lax.axis_index("row") * 16 + lax.axis_index("col")
    x, y, z, core = spot
    first_row = lax.axis_index("row") * 96
    first_col = lax.axis_index("col") * 48
    lane = lax.broadcasted_iota(jnp.int32, (1, 768), 1)
    in_row = lax.rem(lane, 96)
    in_col = lane // 96
    row_valid = jnp.zeros((1, 768), jnp.int32)
    for i in range(96):
        row_valid = jnp.where(in_row == i, valid_ref[first_row + i], row_valid)
    for s in range(6):
        col_valid = jnp.zeros((1, 768), jnp.int32)
        for j in range(8):
            col_valid = jnp.where(in_col == j, valid_ref[first_col + s * 8 + j], col_valid)
        mask_ref[:, s * 768 : s * 768 + 768] = (row_valid * col_valid).astype(F32)

    def wide(s):
        return pl.ds(pl.multiple_of(s * 768, 768), 768)

    def weight(n, hi=th, lo=tl):
        rows = pl.ds(n * 128, 128)
        return hi[rows, :], lo[rows, :]

    def side(n, lanes, lin_ref, sig_ref, out_ref):
        normed = (nh[:, lanes], nl[:, lanes])
        lin = dot3(weight(n), normed, NN)
        sig = sigmoid(dot3(weight(n + 1), normed, NN))
        lin_ref[:, lanes] = lin
        sig_ref[:, lanes] = sig
        out_ref[:, lanes] = mask_ref[:, lanes] * sig * lin

    which = iter(range(SENDS))

    def send(src, dst, part):
        n = next(which)
        lanes = lanes_of(part)
        send_all(src, dst, lanes, send_sem.at[n], recv_sem.at[n])
        return (
            lambda: wait_all(tally, part, send_sem.at[n]),
            lambda: wait_all(tally, part, recv_sem.at[n]),
        )

    moves_r = []
    for i, part in enumerate(B_PARTS):

        @chunks_of(part)
        def _(s):
            lanes = wide(s)
            pltpu.make_async_copy(pair_hbm.at[:, s], xin.at[s], in_sem.at[s]).wait()
            hat, inv = norm_parts(turn_in(xin.at[s]))
            hat_ref[:, lanes] = hat
            inv_ref[:, lanes] = inv
            nh[:, lanes], nl[:, lanes] = split(hat * gain_in)
            side(2, lanes, lb, sb, s2)

        if i == 0:
            pl.semaphore_wait(barrier, 127)
        moves_r.append(send(s2, r2, part))
    moves = []
    for part in A_PARTS:

        @chunks_of(part)
        def _(s):
            side(0, wide(s), la, sa, s1)

        moves.append(send(s1, r1, part))

    @chunks_of(ALL)
    def _(s):
        lanes = wide(s)
        sg[:, lanes] = sigmoid(dot3(weight(4), (nh[:, lanes], nl[:, lanes]), NN))

    for i, part in enumerate(B_PARTS):
        moves_r[i][1]()
        gather_matrix(r2, bh, bl, part)
    for i, part in enumerate(A_PARTS):
        moves[i][1]()
        gather_matrix(r1, ah, al, part)
        rows = rows_of(part)

        @pl.loop(0, 3)
        def _(n):
            lanes = pl.ds(pl.multiple_of(n * 256, 256), 256)
            got = dot3((bh[rows, :], bl[rows, :]), (ah[rows, lanes], al[rows, lanes]), TN)
            if i > 0:
                got = got + res[:, lanes]
            if i < len(A_PARTS) - 1:
                res[:, lanes] = got
            else:
                for t in range(2):
                    for q in range(16):
                        scr[n * 2 + t, pl.ds(q * PITCH, 48), :] = got[
                            q * 48 : q * 48 + 48, t * 128 : t * 128 + 128
                        ]

    for out, _in in moves:
        out()
    moves = []
    for part in T_PARTS:
        spread_pitched(scr, s1, part)
        moves.append(send(s1, r3, part))

    for out, _in in moves_r:
        out()
    later = []
    for i, part in enumerate(T_PARTS):
        moves[i][1]()

        @chunks_of(part)
        def _(s):
            lanes = wide(s)
            pltpu.make_async_copy(go_hbm.at[:, s], gin.at[s], go_sem.at[s]).wait()
            tri_hat, tri_inv = norm_parts(r3[:, lanes])
            tri_norm = split(tri_hat * gain_tri)
            lin_o = dot3(weight(5), tri_norm, NN)
            sig = sg[:, lanes]
            d_out = turn_in(gin.at[s]) * sig
            dg[:, lanes] = d_out * lin_o * (1.0 - sig)
            d_out = split(d_out)
            d_norm = dot3(weight(5, uh, ul), d_out, NN)
            s2[:, lanes] = norm_back(d_norm * gain_tri, tri_hat, tri_inv)
            gw_ref[pl.ds(640, 128), :] += dot3(tri_norm, d_out, NT)
            prod = d_norm * tri_hat
            g2_ref[...] += sum(prod[:, 128 * t : 128 * t + 128] for t in range(6))

        later.append(send(s2, r2, part))

    def use(n, lanes, grad):
        grad = split(grad)
        rows = pl.ds(n * 128, 128)
        gw_ref[rows, :] += dot3((nh[:, lanes], nl[:, lanes]), grad, NT)
        return dot3(weight(n, uh, ul), grad, NN)

    @chunks_of(ALL)
    def _(s):
        lanes = wide(s)
        sg[:, lanes] = use(4, lanes, dg[:, lanes])

    for i, part in enumerate(T_PARTS):
        later[i][1]()
        gather_pitched(r2, scr, part)
        first, many = part[0] * 8, (part[1] - part[0]) * 8

        @pl.loop(0, 16)
        def _(q):
            for t in range(6):
                hi, lo = split(scr[t, pl.ds(pl.multiple_of(q * PITCH + first, 8), many), :])
                rows = pl.ds(pl.multiple_of(q * 48 + first, 16), many)
                dh[rows, pl.ds(t * 128, 128)] = hi
                dl[rows, pl.ds(t * 128, 128)] = lo

    for out, _in in moves:
        out()
    moves_a = []
    for part in DA_PARTS:
        rows = rows_of(part)

        @pl.loop(0, 3)
        def _(n):
            lanes = pl.ds(pl.multiple_of(n * 256, 256), 256)
            res[rows, lanes] = dot3((bh[rows, :], bl[rows, :]), (dh[:, lanes], dl[:, lanes]), NN)

        spread_rows(res, s1, part)
        moves_a.append(send(s1, r1, part))
    for out, _in in later:
        out()
    moves_b = []
    for part in DB_PARTS:
        rows = rows_of(part)

        @pl.loop(0, 3)
        def _(n):
            lanes = pl.ds(pl.multiple_of(n * 256, 256), 256)
            res[rows, lanes] = dot3((ah[rows, :], al[rows, :]), (dh[lanes, :], dl[lanes, :]), NT)

        spread_rows(res, s2, part)
        moves_b.append(send(s2, r3, part))

    def back(n, lanes, d_ref, lin_ref, sig_ref):
        sig = sig_ref[:, lanes]
        d_lin = d_ref[:, lanes] * mask_ref[:, lanes] * sig
        first = use(n, lanes, d_lin)
        return first + use(n + 1, lanes, d_lin * lin_ref[:, lanes] * (1.0 - sig))

    for i, part in enumerate(DA_PARTS):
        moves_a[i][1]()

        @chunks_of(part)
        def _(s):
            lanes = wide(s)
            sg[:, lanes] += back(0, lanes, r1, la, sa)

    def source_row(tile):
        return tile * 8 + (tile // 32) * 256

    def early_tile(x, y, z):
        return (x * 4 + y) * 4 + z

    for a, b, c in CHIPS:
        tx, ty, tz = chip_at(spot, a, b, c)
        rows = pl.ds(pl.multiple_of(source_row(early_tile(tx, ty, tz)), 8), 8)
        copy = tile_copy(
            gw_ref.at[rows, :], parts1.at[eight(me), :], sum_send.at[0], sum_recv.at[0],
            device_at(tx, ty, tz, 0),
        )
        if (a, b, c) == (0, 0, 0):
            pl.when(core == 1)(copy.start)
        else:
            copy.start()

    early_rows = pl.ds(pl.multiple_of(source_row(early_tile(x, y, z)), 8), 8)

    def reduce_tile(src_rows, parts, out_ref, out_rows, n):
        parts[eight(me), :] = gw_ref[src_rows, :]
        wait_tiles(parts, 127, sum_recv.at[n])
        total = parts[...].reshape(128, 8, 128).sum(0) * (1.0 / 768)
        mine[...] = total
        out_ref[out_rows, :] = total
        for step in steps():
            tile_copy(
                mine, out_ref.at[out_rows, :], sum_send.at[n + 1], sum_recv.at[n + 1],
                partner(spot, step),
            ).start()

    def early_reduce():
        @pl.when(core == 0)
        def _():
            reduce_tile(early_rows, parts1, wo_ref, early_rows, 0)

    late_z = (z // 2) * 2
    late_owner = jnp.logical_and(core == 1, lax.rem(z, 2) == 0)
    gain_x, gain_y, gain_z, gain_core = 0, 0, 1, 1
    gain_device = device_at(gain_x, gain_y, gain_z, gain_core)
    gain_me = gain_device[0] * 16 + gain_device[1]
    gain_owner = me == gain_me

    def late_row(x, y, z):
        return pl.multiple_of(256 + ((x * 4 + y) * 2 + z // 2) * 8, 8)

    def late_send():
        for a, b, c in CHIPS:
            if c % 2:
                continue
            tx, ty, tz = lax.rem(x + a, 4), lax.rem(y + b, 4), lax.rem(late_z + c, 4)
            copy = tile_copy(
                gw_ref.at[pl.ds(late_row(tx, ty, tz), 8), :], parts2.at[eight(me), :],
                sum_send.at[2], sum_recv.at[2], device_at(tx, ty, tz, 1),
            )
            if (a, b, c) == (0, 0, 0):
                pl.when(jnp.logical_not(late_owner))(copy.start)
            else:
                copy.start()
        for n, ref in ((0, g1_ref), (1, g2_ref)):
            gw_ref[pl.ds(768 + n, 1), :] = jnp.sum(ref[...].T, axis=0, keepdims=True)
        pl.when(jnp.logical_not(gain_owner))(
            tile_copy(
                gw_ref.at[pl.ds(768, 8), :], parts2.at[eight(me), :],
                sum_send.at[4], sum_recv.at[4], gain_device,
            ).start
        )

    for i, part in enumerate(DB_PARTS):
        moves_b[i][1]()
        last = i == len(DB_PARTS) - 1

        @chunks_of(part)
        def _(s):
            lanes = wide(s)
            total = sg[:, lanes] + back(2, lanes, r3, lb, sb)
            hat = hat_ref[:, lanes]
            prod = total * hat
            g1_ref[...] += sum(prod[:, 128 * t : 128 * t + 128] for t in range(6))
            sg[:, lanes] = total

        if last:
            late_send()

        @chunks_of(part)
        def _(s):
            lanes = wide(s)
            grad = norm_back(sg[:, lanes] * gain_in, hat_ref[:, lanes], inv_ref[:, lanes]).T
            flat = xin.at[s].reshape(768, 128)
            for j in range(8):
                flat[pl.ds(j, 96, stride=8), :] = grad[j * 96 : (j + 1) * 96, :]
            pltpu.make_async_copy(xin.at[s], gp_hbm.at[:, s], out_sem.at[s]).start()

        if i == 0:
            early_reduce()

    late_rows = pl.ds(late_row(x, y, late_z), 8)

    @pl.when(late_owner)
    def _():
        reduce_tile(late_rows, parts2, wo_ref, late_rows, 2)

    @pl.when(gain_owner)
    def _():
        reduce_tile(pl.ds(768, 8), parts2, go_ref, pl.ds(0, 8), 4)

    for out, _in in moves_a + moves_b:
        out()
    for s in range(6):
        pltpu.make_async_copy(xin.at[s], gp_hbm.at[:, s], out_sem.at[s]).wait()

    settle(gw_ref, parts1, 64, core == 0, sum_send, sum_recv, 0)
    settle(gw_ref, parts1, 32, late_owner, sum_send, sum_recv, 2)
    settle(gw_ref, parts1, 1, gain_owner, sum_send, sum_recv, 4)


def whole_step(pair4, go4, valid, gains, weights):
    vmem = pl.BlockSpec(memory_space=pltpu.VMEM)
    hbm = pl.BlockSpec(memory_space=pl.ANY)
    full = pltpu.VMEM((128, 4608), F32)
    half = pltpu.VMEM((128, 4608), BF16)
    mat = pltpu.VMEM((768, 768), BF16)
    wts = pltpu.VMEM((768, 128), BF16)
    tiles = pltpu.VMEM((6, 96, 8, 128), F32)
    dma = pltpu.SemaphoreType.DMA
    square = pltpu.VMEM((128, 128), F32)
    return pl.pallas_call(
        step_kernel,
        in_specs=[hbm, hbm, pl.BlockSpec(memory_space=pltpu.SMEM), vmem, vmem],
        out_specs=[hbm, vmem, vmem],
        out_shape=[
            jax.ShapeDtypeStruct((96, 6, 8, 128), F32),
            jax.ShapeDtypeStruct((768, 128), F32),
            jax.ShapeDtypeStruct((8, 128), F32),
        ],
        scratch_shapes=[tiles, tiles, full, full, full, full, full, full]
        + [pltpu.VMEM((1, 4608), F32), half, half]
        + [full] * 6
        + [mat] * 6
        + [pltpu.VMEM((768, 768), F32), pltpu.VMEM((6, 16 * PITCH, 128), F32)]
        + [wts] * 4
        + [pltpu.VMEM((762, 6, 128), F32)]
        + [pltpu.VMEM((1, 4608), F32), pltpu.VMEM((776, 128), F32), square, square]
        + [pltpu.VMEM((2, 128, 128), F32)]
        + [pltpu.VMEM((1024, 128), F32)] * 2
        + [pltpu.VMEM((8, 128), F32)]
        + [dma((6,)), dma((6,)), dma((6,)), dma((SENDS,)), dma((SENDS,))]
        + [dma((6,)), dma((6,))],
        compiler_params=params(collective_id=0, has_side_effects=True),
        name="whole_step",
    )(pair4, go4, valid, gains, weights)


def on_device(pair_act, grad_out, residue_mask, norm_gains, weights):
    tile_rows, tile_cols, channels = pair_act.shape
    pair4 = pair_act.reshape(tile_rows, tile_cols // 8, 8, channels)
    go4 = grad_out.reshape(tile_rows, tile_cols // 8, 8, channels)
    grad_pair, grad_weights, grad_gains = whole_step(
        pair4, go4, residue_mask, norm_gains, weights
    )
    return (
        grad_pair.reshape(pair_act.shape),
        grad_weights.reshape(weights.shape),
        grad_gains[: norm_gains.shape[0]],
    )


def solution(mesh):
    return jax.shard_map(
        on_device,
        mesh=mesh,
        in_specs=(P("row", "col", None), P("row", "col", None), P(), P(), P()),
        out_specs=(P("row", "col", None), P(), P()),
        check_vma=False,
    )
```

```python
import functools

import jax
import jax.numpy as jnp
from jax import lax
from jax.experimental import pallas as pl
from jax.experimental.pallas import tpu as pltpu
from jax.sharding import PartitionSpec as P

EPS = 1e-05
F32 = jnp.float32
BF16 = jnp.bfloat16
MESH = pl.DeviceIdType.MESH
VLIM = 60 * 2**20


def params(**kw):
    return pltpu.CompilerParams(vmem_limit_bytes=VLIM, **kw)


def split(v):
    hi = v.astype(BF16)
    lo = (v - hi.astype(F32)).astype(BF16)
    return hi, lo


def dot3(lhs, rhs, dims):
    (lh, ll), (rh, rl) = lhs, rhs
    d = functools.partial(
        lax.dot_general, dimension_numbers=(dims, ((), ())), preferred_element_type=F32
    )
    return d(lh, rh) + (d(lh, rl) + d(ll, rh))


NN = ((1,), (0,))
NT = ((1,), (1,))
TN = ((0,), (0,))


def place():
    row = lax.axis_index("row")
    col = lax.axis_index("col")
    return row // 2, col // 4, lax.rem(row, 2) * 2 + lax.rem(col // 2, 2), lax.rem(col, 2)


def partner(spot, step):
    x, y, z, core = spot
    a, b, c, d = step
    x = lax.rem(x + a, 4)
    y = lax.rem(y + b, 4)
    z = lax.rem(z + c, 4)
    core = lax.rem(core + d, 2)
    return x * 2 + z // 2, y * 4 + lax.rem(z, 2) * 2 + core


def steps():
    out = []
    for s in range(1, 128):
        o = (s * 45) % 128
        out.append((o // 2 % 4, o // 8 % 4, o // 32, o % 2))
    return out


def row_of(ref, row, lanes):
    return ref.at[pl.ds(row, 1), lanes]


def send_all(src, dst, lanes, send_sem, recv_sem):
    spot = place()
    me = lax.axis_index("row") * 16 + lax.axis_index("col")
    for step in steps():
        r, q = partner(spot, step)
        pltpu.make_async_remote_copy(
            src_ref=row_of(src, r * 16 + q, lanes),
            dst_ref=row_of(dst, me, lanes),
            send_sem=send_sem,
            recv_sem=recv_sem,
            device_id={"row": r, "col": q},
            device_id_type=MESH,
        ).start()
    dst[pl.ds(me, 1), lanes] = src[pl.ds(me, 1), lanes]


def wait_all(tally, part, sem):
    some = tally.at[pl.ds(0, 127 * (part[1] - part[0]))]
    pltpu.make_async_copy(some, some, sem).wait()


def chip_at(spot, a, b, c):
    x, y, z, _ = spot
    return lax.rem(x + a, 4), lax.rem(y + b, 4), lax.rem(z + c, 4)


def device_at(x, y, z, core):
    return x * 2 + z // 2, y * 4 + lax.rem(z, 2) * 2 + core


def eight(tile):
    return pl.ds(pl.multiple_of(tile * 8, 8), 8)


def tile_copy(src, dst, send_sem, recv_sem, device):
    return pltpu.make_async_remote_copy(
        src_ref=src,
        dst_ref=dst,
        send_sem=send_sem,
        recv_sem=recv_sem,
        device_id={"row": device[0], "col": device[1]},
        device_id_type=MESH,
    )


def wait_tiles(ref, count, sem):
    some = ref.at[pl.ds(0, count * 8), :]
    pltpu.make_async_copy(some, some, sem).wait()


def settle(small, large, tiles, owner, send_sem, recv_sem, n):
    @pl.when(owner)
    def _():
        if tiles > 1:
            wait_tiles(small, tiles - 1, send_sem.at[n])
            wait_tiles(small, tiles - 1, recv_sem.at[n + 1])
        wait_tiles(large, 127, send_sem.at[n + 1])

    @pl.when(jnp.logical_not(owner))
    def _():
        wait_tiles(small, tiles, send_sem.at[n])
        wait_tiles(small, tiles, recv_sem.at[n + 1])


CHIPS = [(o // 16, o // 4 % 4, o % 4) for o in [(s * 27) % 64 for s in range(64)]]


def turn_in(ref):
    rows = ref.shape[0]
    flat = ref.reshape(rows * 8, 128)
    parts = [flat[pl.ds(j, rows, stride=8), :] for j in range(8)]
    return jnp.concatenate(parts, axis=0).T


def norm_parts(v):
    scale = 1.0 / v.shape[0]
    mu = jnp.sum(v, axis=0, keepdims=True) * scale
    cen = v - mu
    inv = lax.rsqrt(jnp.sum(cen * cen, axis=0, keepdims=True) * scale + EPS)
    return cen * inv, inv


def norm_back(h, hat, inv):
    scale = 1.0 / h.shape[0]
    m1 = jnp.sum(h, axis=0, keepdims=True) * scale
    m2 = jnp.sum(h * hat, axis=0, keepdims=True) * scale
    return inv * (h - m1 - hat * m2)


def sigmoid(v):
    return 1.0 / (1.0 + jnp.exp(-v))


def swap_four(blocks):
    lane = lax.broadcasted_iota(jnp.int32, blocks[0].shape, 1)
    outs = []
    for a in range(4):
        out = None
        for b in range(4):
            shift = (96 * (b - a)) % 384
            moved = blocks[b] if shift == 0 else pltpu.roll(blocks[b], shift, 1)
            out = moved if out is None else jnp.where(lane < 96 * b, out, moved)
        outs.append(out)
    return outs


def read_group(ref, group, half):
    lanes = pl.ds(pl.multiple_of(group * 384, 384), 384)
    return [ref[pl.ds((half * 4 + r) * 16, 16), lanes] for r in range(4)]


def write_group(ref, group, half, blocks):
    lanes = pl.ds(pl.multiple_of(group * 384, 384), 384)
    for r in range(4):
        ref[pl.ds((half * 4 + r) * 16, 16), lanes] = blocks[r]


PITCH = 56
UNIT = 768


def lanes_of(part):
    return pl.ds(part[0] * UNIT, (part[1] - part[0]) * UNIT)


def groups_of(part):
    return pl.loop(part[0] * 2, part[1] * 2)


def chunks_of(part):
    return pl.loop(part[0], part[1])


def rows_of(part):
    return pl.ds(part[0] * 128, (part[1] - part[0]) * 128)


def gather_matrix(src_ref, hi_ref, lo_ref, part):
    @groups_of(part)
    def _(group):
        for half in range(2):
            for k, block in enumerate(swap_four(read_group(src_ref, group, half))):
                hi, lo = split(block)
                rows = pl.ds(pl.multiple_of(group * 64 + k * 16, 16), 16)
                lanes = pl.ds(half * 384, 384)
                hi_ref[rows, lanes] = hi
                lo_ref[rows, lanes] = lo


def spread_pitched(scr, out_ref, part):
    @groups_of(part)
    def _(group):
        for half in range(2):
            blocks = []
            for k in range(4):
                pieces = [
                    scr.at[half * 3 + t][pl.ds(group * 4 + k, 16, stride=PITCH), :]
                    for t in range(3)
                ]
                blocks.append(jnp.concatenate(pieces, axis=1))
            write_group(out_ref, group, half, swap_four(blocks))


def spread_rows(res, out_ref, part):
    @groups_of(part)
    def _(group):
        for half in range(2):
            blocks = [
                res[
                    pl.ds(pl.multiple_of(group * 64 + k * 16, 16), 16),
                    pl.ds(half * 384, 384),
                ]
                for k in range(4)
            ]
            write_group(out_ref, group, half, swap_four(blocks))


def gather_pitched(src_ref, scr, part):
    @groups_of(part)
    def _(group):
        for half in range(2):
            for k, block in enumerate(swap_four(read_group(src_ref, group, half))):
                for t in range(3):
                    scr.at[half * 3 + t][pl.ds(group * 4 + k, 16, stride=PITCH), :] = block[
                        :, t * 128 : t * 128 + 128
                    ]


B_PARTS = ((0, 2), (2, 6))
A_PARTS = ((0, 4), (4, 6))
T_PARTS = ((0, 2), (2, 4), (4, 6))
DA_PARTS = ((0, 2), (2, 6))
DB_PARTS = ((0, 3), (3, 5), (5, 6))
ALL = (0, 6)
SENDS = 15


def step_kernel(
    pair_hbm, go_hbm, valid_ref, gain_ref, w_ref, gp_hbm, wo_ref, gains_out,
    xin, gin, s1, s2, r1, r2, r3, hat_ref, inv_ref, nh, nl, la, sa, lb, sb, sg, dg,
    ah, al, bh, bl, th_b, tl_b, dh, dl, res, scr, th, tl, uh, ul, tally,
    mask_ref, gw_ref, g1_ref, g2_ref, gains, parts1, parts2, mine, go_ref,
    in_sem, go_sem, out_sem, send_sem, recv_sem, sum_send, sum_recv,
):
    spot = place()
    for s in range(6):
        pltpu.make_async_copy(pair_hbm.at[:, s], xin.at[s], in_sem.at[s]).start()
    for s in range(6):
        pltpu.make_async_copy(go_hbm.at[:, s], gin.at[s], go_sem.at[s]).start()
    barrier = pltpu.get_barrier_semaphore()
    for step in steps():
        r, q = partner(spot, step)
        pl.semaphore_signal(
            barrier, inc=1, device_id={"row": r, "col": q}, device_id_type=MESH
        )
    def prepare(n):
        rows = pl.ds(n * 128, 128)
        th[rows, :], tl[rows, :] = split(w_ref[n].T)
        uh[rows, :], ul[rows, :] = split(w_ref[n])

    prepare(2)
    prepare(3)
    gw_ref[...] = jnp.zeros_like(gw_ref)
    g1_ref[...] = jnp.zeros_like(g1_ref)
    g2_ref[...] = jnp.zeros_like(g2_ref)
    for n in range(2):
        gains[n] = jnp.broadcast_to(gain_ref[n : n + 1, :], (128, 128)).T
    gain_in = gains[0, :, 0:1]
    gain_tri = gains[1, :, 0:1]
    me = lax.axis_index("row") * 16 + lax.axis_index("col")
    x, y, z, core = spot
    first_row = lax.axis_index("row") * 96
    first_col = lax.axis_index("col") * 48
    lane = lax.broadcasted_iota(jnp.int32, (1, 768), 1)
    in_row = lax.rem(lane, 96)
    in_col = lane // 96
    row_valid = jnp.zeros((1, 768), jnp.int32)
    for i in range(96):
        row_valid = jnp.where(in_row == i, valid_ref[first_row + i], row_valid)
    for s in range(6):
        col_valid = jnp.zeros((1, 768), jnp.int32)
        for j in range(8):
            col_valid = jnp.where(in_col == j, valid_ref[first_col + s * 8 + j], col_valid)
        mask_ref[:, s * 768 : s * 768 + 768] = (row_valid * col_valid).astype(F32)

    def wide(s):
        return pl.ds(pl.multiple_of(s * 768, 768), 768)

    def weight(n, hi=th, lo=tl):
        rows = pl.ds(n * 128, 128)
        return hi[rows, :], lo[rows, :]

    def side(n, lanes, lin_ref, sig_ref, out_ref):
        normed = (nh[:, lanes], nl[:, lanes])
        lin = dot3(weight(n), normed, NN)
        sig = sigmoid(dot3(weight(n + 1), normed, NN))
        lin_ref[:, lanes] = lin
        sig_ref[:, lanes] = sig
        out_ref[:, lanes] = mask_ref[:, lanes] * sig * lin

    which = iter(range(SENDS))

    def send(src, dst, part):
        n = next(which)
        lanes = lanes_of(part)
        send_all(src, dst, lanes, send_sem.at[n], recv_sem.at[n])
        return (
            lambda: wait_all(tally, part, send_sem.at[n]),
            lambda: wait_all(tally, part, recv_sem.at[n]),
        )

    moves_r = []
    for i, part in enumerate(B_PARTS):

        @chunks_of(part)
        def _(s):
            lanes = wide(s)
            pltpu.make_async_copy(pair_hbm.at[:, s], xin.at[s], in_sem.at[s]).wait()
            hat, inv = norm_parts(turn_in(xin.at[s]))
            hat_ref[:, lanes] = hat
            inv_ref[:, lanes] = inv
            nh[:, lanes], nl[:, lanes] = split(hat * gain_in)
            side(2, lanes, lb, sb, s2)

        if i == 0:
            pl.semaphore_wait(barrier, 127)
        moves_r.append(send(s2, r2, part))
        if i == 0:
            for n in (0, 1, 4, 5):
                prepare(n)
    moves = []
    for part in A_PARTS:

        @chunks_of(part)
        def _(s):
            side(0, wide(s), la, sa, s1)

        moves.append(send(s1, r1, part))

    @chunks_of(ALL)
    def _(s):
        lanes = wide(s)
        sg[:, lanes] = sigmoid(dot3(weight(4), (nh[:, lanes], nl[:, lanes]), NN))

    for i, part in enumerate(B_PARTS):
        moves_r[i][1]()
        gather_matrix(r2, bh, bl, part)

        @chunks_of(part)
        def _(s):
            here = pl.ds(pl.multiple_of(s * 128, 128), 128)
            for src, out in ((bh, th_b), (bl, tl_b)):
                for j in range(6):
                    there = pl.ds(j * 128, 128)
                    out[there, here] = src[here, there].T

    for i, part in enumerate(A_PARTS):
        moves[i][1]()
        gather_matrix(r1, ah, al, part)
        rows = rows_of(part)

        @pl.loop(0, 3)
        def _(n):
            lanes = pl.ds(pl.multiple_of(n * 256, 256), 256)
            got = dot3(
                (th_b[:, rows], tl_b[:, rows]), (ah[rows, lanes], al[rows, lanes]), NN
            )
            if i > 0:
                got = got + res[:, lanes]
            if i < len(A_PARTS) - 1:
                res[:, lanes] = got
            else:
                for t in range(2):
                    for q in range(16):
                        scr[n * 2 + t, pl.ds(q * PITCH, 48), :] = got[
                            q * 48 : q * 48 + 48, t * 128 : t * 128 + 128
                        ]

    for out, _in in moves:
        out()
    moves = []
    for part in T_PARTS:
        spread_pitched(scr, s1, part)
        moves.append(send(s1, r3, part))

    for out, _in in moves_r:
        out()
    later = []
    for i, part in enumerate(T_PARTS):
        moves[i][1]()

        @chunks_of(part)
        def _(s):
            lanes = wide(s)
            pltpu.make_async_copy(go_hbm.at[:, s], gin.at[s], go_sem.at[s]).wait()
            tri_hat, tri_inv = norm_parts(r3[:, lanes])
            tri_norm = split(tri_hat * gain_tri)
            lin_o = dot3(weight(5), tri_norm, NN)
            sig = sg[:, lanes]
            d_out = turn_in(gin.at[s]) * sig
            dg[:, lanes] = d_out * lin_o * (1.0 - sig)
            d_out = split(d_out)
            d_norm = dot3(weight(5, uh, ul), d_out, NN)
            s2[:, lanes] = norm_back(d_norm * gain_tri, tri_hat, tri_inv)
            gw_ref[pl.ds(640, 128), :] += dot3(tri_norm, d_out, NT)
            prod = d_norm * tri_hat
            g2_ref[...] += sum(prod[:, 128 * t : 128 * t + 128] for t in range(6))

        later.append(send(s2, r2, part))

    def use(n, lanes, grad):
        grad = split(grad)
        rows = pl.ds(n * 128, 128)
        gw_ref[rows, :] += dot3((nh[:, lanes], nl[:, lanes]), grad, NT)
        return dot3(weight(n, uh, ul), grad, NN)

    @chunks_of(ALL)
    def _(s):
        lanes = wide(s)
        sg[:, lanes] = use(4, lanes, dg[:, lanes])

    for i, part in enumerate(T_PARTS):
        later[i][1]()
        gather_pitched(r2, scr, part)
        first, many = part[0] * 8, (part[1] - part[0]) * 8

        @pl.loop(0, 16)
        def _(q):
            for t in range(6):
                hi, lo = split(scr[t, pl.ds(pl.multiple_of(q * PITCH + first, 8), many), :])
                rows = pl.ds(pl.multiple_of(q * 48 + first, 16), many)
                dh[rows, pl.ds(t * 128, 128)] = hi
                dl[rows, pl.ds(t * 128, 128)] = lo

    for out, _in in moves:
        out()
    moves_a = []
    for part in DA_PARTS:
        rows = rows_of(part)

        @pl.loop(0, 3)
        def _(n):
            lanes = pl.ds(pl.multiple_of(n * 256, 256), 256)
            res[rows, lanes] = dot3((bh[rows, :], bl[rows, :]), (dh[:, lanes], dl[:, lanes]), NN)

        spread_rows(res, s1, part)
        moves_a.append(send(s1, r1, part))
    for out, _in in later:
        out()
    moves_b = []
    for part in DB_PARTS:
        rows = rows_of(part)

        @pl.loop(0, 3)
        def _(n):
            lanes = pl.ds(pl.multiple_of(n * 256, 256), 256)
            res[rows, lanes] = dot3((ah[rows, :], al[rows, :]), (dh[lanes, :], dl[lanes, :]), NT)

        spread_rows(res, s2, part)
        moves_b.append(send(s2, r3, part))

    def back(n, lanes, d_ref, lin_ref, sig_ref):
        sig = sig_ref[:, lanes]
        d_lin = d_ref[:, lanes] * mask_ref[:, lanes] * sig
        first = use(n, lanes, d_lin)
        return first + use(n + 1, lanes, d_lin * lin_ref[:, lanes] * (1.0 - sig))

    for i, part in enumerate(DA_PARTS):
        moves_a[i][1]()

        @chunks_of(part)
        def _(s):
            lanes = wide(s)
            sg[:, lanes] += back(0, lanes, r1, la, sa)

    def source_row(tile):
        return tile * 8 + (tile // 32) * 256

    def early_tile(x, y, z):
        return (x * 4 + y) * 4 + z

    for a, b, c in CHIPS:
        tx, ty, tz = chip_at(spot, a, b, c)
        rows = pl.ds(pl.multiple_of(source_row(early_tile(tx, ty, tz)), 8), 8)
        copy = tile_copy(
            gw_ref.at[rows, :], parts1.at[eight(me), :], sum_send.at[0], sum_recv.at[0],
            device_at(tx, ty, tz, 0),
        )
        if (a, b, c) == (0, 0, 0):
            pl.when(core == 1)(copy.start)
        else:
            copy.start()

    early_rows = pl.ds(pl.multiple_of(source_row(early_tile(x, y, z)), 8), 8)

    def reduce_tile(src_rows, parts, out_ref, out_rows, n):
        parts[eight(me), :] = gw_ref[src_rows, :]
        wait_tiles(parts, 127, sum_recv.at[n])
        total = parts[...].reshape(128, 8, 128).sum(0) * (1.0 / 768)
        mine[...] = total
        out_ref[out_rows, :] = total
        for step in steps():
            tile_copy(
                mine, out_ref.at[out_rows, :], sum_send.at[n + 1], sum_recv.at[n + 1],
                partner(spot, step),
            ).start()

    def early_reduce():
        @pl.when(core == 0)
        def _():
            reduce_tile(early_rows, parts1, wo_ref, early_rows, 0)

    late_z = (z // 2) * 2
    late_owner = jnp.logical_and(core == 1, lax.rem(z, 2) == 0)
    gain_x, gain_y, gain_z, gain_core = 0, 0, 1, 1
    gain_device = device_at(gain_x, gain_y, gain_z, gain_core)
    gain_me = gain_device[0] * 16 + gain_device[1]
    gain_owner = me == gain_me

    def late_row(x, y, z):
        return pl.multiple_of(256 + ((x * 4 + y) * 2 + z // 2) * 8, 8)

    def late_send():
        for a, b, c in CHIPS:
            if c % 2:
                continue
            tx, ty, tz = lax.rem(x + a, 4), lax.rem(y + b, 4), lax.rem(late_z + c, 4)
            copy = tile_copy(
                gw_ref.at[pl.ds(late_row(tx, ty, tz), 8), :], parts2.at[eight(me), :],
                sum_send.at[2], sum_recv.at[2], device_at(tx, ty, tz, 1),
            )
            if (a, b, c) == (0, 0, 0):
                pl.when(jnp.logical_not(late_owner))(copy.start)
            else:
                copy.start()
        for n, ref in ((0, g1_ref), (1, g2_ref)):
            gw_ref[pl.ds(768 + n, 1), :] = jnp.sum(ref[...].T, axis=0, keepdims=True)
        pl.when(jnp.logical_not(gain_owner))(
            tile_copy(
                gw_ref.at[pl.ds(768, 8), :], parts2.at[eight(me), :],
                sum_send.at[4], sum_recv.at[4], gain_device,
            ).start
        )

    for i, part in enumerate(DB_PARTS):
        moves_b[i][1]()
        last = i == len(DB_PARTS) - 1

        @chunks_of(part)
        def _(s):
            lanes = wide(s)
            total = sg[:, lanes] + back(2, lanes, r3, lb, sb)
            hat = hat_ref[:, lanes]
            prod = total * hat
            g1_ref[...] += sum(prod[:, 128 * t : 128 * t + 128] for t in range(6))
            sg[:, lanes] = total

        if last:
            late_send()

        @chunks_of(part)
        def _(s):
            lanes = wide(s)
            grad = norm_back(sg[:, lanes] * gain_in, hat_ref[:, lanes], inv_ref[:, lanes]).T
            flat = gp_hbm.at[s].reshape(768, 128)
            for j in range(8):
                flat[pl.ds(j, 96, stride=8), :] = grad[j * 96 : (j + 1) * 96, :]

        if last:
            early_reduce()

    late_rows = pl.ds(late_row(x, y, late_z), 8)

    @pl.when(late_owner)
    def _():
        reduce_tile(late_rows, parts2, wo_ref, late_rows, 2)

    @pl.when(gain_owner)
    def _():
        reduce_tile(pl.ds(768, 8), parts2, go_ref, pl.ds(0, 8), 4)

    for out, _in in moves_a + moves_b:
        out()

    settle(gw_ref, parts1, 64, core == 0, sum_send, sum_recv, 0)
    settle(gw_ref, parts1, 32, late_owner, sum_send, sum_recv, 2)
    settle(gw_ref, parts1, 1, gain_owner, sum_send, sum_recv, 4)
    gains_out[...] = go_ref[0:2, :]


def whole_step(pair4, go4, valid, gains, weights):
    vmem = pl.BlockSpec(memory_space=pltpu.VMEM)
    hbm = pl.BlockSpec(memory_space=pl.ANY)
    full = pltpu.VMEM((128, 4608), F32)
    half = pltpu.VMEM((128, 4608), BF16)
    mat = pltpu.VMEM((768, 768), BF16)
    wts = pltpu.VMEM((768, 128), BF16)
    tiles = pltpu.VMEM((6, 96, 8, 128), F32)
    dma = pltpu.SemaphoreType.DMA
    square = pltpu.VMEM((128, 128), F32)
    return pl.pallas_call(
        step_kernel,
        in_specs=[hbm, hbm, pl.BlockSpec(memory_space=pltpu.SMEM), vmem, vmem],
        out_specs=[vmem, vmem, vmem],
        out_shape=[
            pltpu.VMEM((6, 96, 8, 128), F32),
            jax.ShapeDtypeStruct((768, 128), F32),
            jax.ShapeDtypeStruct((2, 128), F32),
        ],
        scratch_shapes=[tiles, tiles, full, full, full, full, full, full]
        + [pltpu.VMEM((1, 4608), F32), half, half]
        + [full] * 6
        + [mat] * 8
        + [pltpu.VMEM((768, 768), F32), pltpu.VMEM((6, 16 * PITCH, 128), F32)]
        + [wts] * 4
        + [pltpu.VMEM((762, 6, 128), F32)]
        + [pltpu.VMEM((1, 4608), F32), pltpu.VMEM((776, 128), F32), square, square]
        + [pltpu.VMEM((2, 128, 128), F32)]
        + [pltpu.VMEM((1024, 128), F32)] * 2
        + [pltpu.VMEM((8, 128), F32)] * 2
        + [dma((6,)), dma((6,)), dma((6,)), dma((SENDS,)), dma((SENDS,))]
        + [dma((6,)), dma((6,))],
        compiler_params=params(collective_id=0, has_side_effects=True),
        name="whole_step",
    )(pair4, go4, valid, gains, weights)


def on_device(pair_act, grad_out, residue_mask, norm_gains, weights):
    tile_rows, tile_cols, channels = pair_act.shape
    pair4 = pair_act.reshape(tile_rows, tile_cols // 8, 8, channels)
    go4 = grad_out.reshape(tile_rows, tile_cols // 8, 8, channels)
    grad_pair, grad_weights, grad_gains = whole_step(
        pair4, go4, residue_mask, norm_gains, weights
    )
    return (
        jnp.transpose(grad_pair, (1, 0, 2, 3)).reshape(pair_act.shape),
        grad_weights.reshape(weights.shape),
        grad_gains,
    )


def solution(mesh):
    return jax.shard_map(
        on_device,
        mesh=mesh,
        in_specs=(P("row", "col", None), P("row", "col", None), P(), P(), P()),
        out_specs=(P("row", "col", None), P(), P()),
        check_vma=False,
    )
```
